32 devices in a mesh: dp: 4 (over y, core), row: 2 (over x), col: 4 (over z).
Axes of the slice: x: 2, y: 2, z: 4, core: 2. Of those that a mesh axis runs over, the one named last changes fastest.
Arguments:
- images: bfloat16 [4, 64, 32, 1024], P('dp', None, 'row', 'col'), may hold values from -6 to 6
- first_kernel: bfloat16 [64, 64, 3, 3], replicated, may hold values from -0.25 to 0.25
- second_kernel: bfloat16 [64, 64, 3, 3], replicated, may hold values from -0.25 to 0.25
- cotangent: bfloat16 [4, 64, 32, 1024], P('dp', None, 'row', 'col'), may hold values from -6 to 6
Outputs:
- outputs: bfloat16 [4, 64, 32, 1024], P('dp', None, 'row', 'col')
- input_grad: bfloat16 [4, 64, 32, 1024], P('dp', None, 'row', 'col')
- first_grad: float32 [64, 64, 3, 3], replicated
- second_grad: float32 [64, 64, 3, 3], replicated
The draws below stay inside these ranges and needn't reach their ends.
All inputs are finite; a program needn't handle non-finite values.
Results may differ from the reference program's by a relative error of at most 0.005.
Values may be sent and summed in bfloat16 or wider, within the bound.
No kernel may reach another device: no remote copies, remote signals or barrier semaphores. Data moves between devices by JAX's collectives and lax.ppermute only.
A program may use at most 64 MiB of HBM per device.

```python
import math
import jax
import jax.numpy as jnp
from jax import lax

C = 64
IMAGES = 4
HEIGHT = 32
WIDTH = 1024


def levels(own_key, extent, cuts, least, high):
    def one(dim, parts):
        draws = jax.random.uniform(jax.random.fold_in(jax.random.fold_in(own_key, 6), dim), (parts,), jnp.float32, least / len(cuts), high / len(cuts))
        return jnp.repeat(jnp.exp(draws), extent[dim] // parts).reshape((-1,) + (1,) * (len(extent) - dim - 1))

    loudness = one(*cuts[0])
    for cut in cuts[1:]:
        loudness = loudness * one(*cut)
    return loudness


def noise(rng, dims, width, reach, shards=(), kind=jnp.bfloat16):
    drawn = jax.random.normal(rng, dims, jnp.float32) * width
    if len(shards) > 0:
        drawn = levels(rng, dims, shards, -0.22, 0.18) * drawn
    return jnp.clip(drawn, min=-reach, max=reach).astype(kind)


def setup_inputs(seed: int = 0) -> dict:
    arg_keys = jax.random.split(jax.random.key(seed), 5)
    images = noise(arg_keys[0], (IMAGES, C, HEIGHT, WIDTH), 1.0, 6.0, ((0, 4), (2, 2), (3, 4)))
    first_kernel = noise(arg_keys[1], (C, C, 3, 3), (9 * C) ** -0.5, 0.25)
    second_kernel = noise(arg_keys[2], (C, C, 3, 3), (9 * C) ** -0.5, 0.25)
    cotangent = noise(arg_keys[3], (IMAGES, C, HEIGHT, WIDTH), 1.0, 6.0, ((0, 4), (2, 2), (3, 4)))
    return dict(images=images, first_kernel=first_kernel, second_kernel=second_kernel, cotangent=cotangent)


def convolve(padded, kernel):
    return lax.conv_general_dilated(padded, kernel, (1, 1), 'VALID', dimension_numbers=('NCHW', 'OIHW', 'NCHW'), preferred_element_type=jnp.float32)

def widen(field):
    return jnp.pad(field, ((0, 0), (0, 0), (1, 1), (1, 1)))

def flipped(kernel):
    return jnp.flip(kernel, (2, 3)).transpose(1, 0, 2, 3)

def silu_grad(value):
    sigma = jax.nn.sigmoid(value)
    return sigma * (1.0 + value * (1.0 - sigma))

def kernel_grad(padded, upstream):
    height = upstream.shape[2]
    breadth = upstream.shape[3]
    outer = []
    for offset_row in range(3):
        inner = []
        for offset_col in range(3):
            window = padded[:, :, offset_row:offset_row + height, offset_col:offset_col + breadth]
            inner.append(jnp.einsum('nihw,nohw->oi', window.astype(jnp.float32), upstream.astype(jnp.float32)))
        outer.append(jnp.stack(inner, -1))
    return jnp.stack(outer, 2)

def reference(images, first_kernel, second_kernel, cotangent):
    factor = 1.0 / math.sqrt(images.shape[0] * images.shape[2] * images.shape[3])

    def single(totals, sample):
        picture = sample[0][None]
        upstream = sample[1][None]
        padded = widen(picture)
        hidden = convolve(padded, first_kernel)
        act_padded = widen(jax.nn.silu(hidden).astype(jnp.bfloat16))
        result = convolve(act_padded, second_kernel).astype(jnp.bfloat16)
        act_grad = convolve(widen(upstream), flipped(second_kernel))
        hid_grad = (act_grad * silu_grad(hidden)).astype(jnp.bfloat16)
        back = convolve(widen(hid_grad), flipped(first_kernel)).astype(jnp.bfloat16)
        first_term = kernel_grad(padded, hid_grad)
        second_term = kernel_grad(act_padded, upstream)
        return ((totals[0] + first_term, totals[1] + second_term), (result[0], back[0]))
    zeros = jnp.zeros(first_kernel.shape, jnp.float32)
    sums, stacked = lax.scan(single, (zeros, zeros), (images, cotangent))
    return (stacked[0], stacked[1], sums[0] * factor, sums[1] * factor)
```

```python
import functools
import math

import jax
import jax.numpy as jnp
from jax import lax
from jax.experimental import pallas as pl
from jax.experimental.pallas import tpu as pltpu
from jax.sharding import PartitionSpec as P

BF = jnp.bfloat16
F32 = jnp.float32
LANES = 128
SLOT = 32
PIECES = 2


def kernel_call(body, outs, scratch=(), flops=0, name=None, **more):
    return pl.pallas_call(
        body,
        out_shape=outs,
        **more,
        scratch_shapes=list(scratch),
        cost_estimate=pl.CostEstimate(flops=flops, transcendentals=0, bytes_accessed=1 << 20),
        compiler_params=pltpu.CompilerParams(vmem_limit_bytes=24 << 20),
        name=name,
    )


def lanes_of(shape):
    return lax.broadcasted_iota(jnp.int32, shape, len(shape) - 1)


def pairs(size, second):
    start = 1 if second else 0
    out = []
    for i in range(start, size - 1, 2):
        out += [(i, i + 1), (i + 1, i)]
    return out


def swap(array, axis, second):
    perm = pairs(lax.axis_size(axis), second)
    if not perm:
        return None
    return lax.ppermute(array, axis, perm)


def pack_body(
    img, cot, k1, k2, x16, own, taps1, taps2, send_a, send_b, row_a, row_b,
    staged, wide, sems, tap_sems,
):
    ch, rows, cols = img.shape[1:]
    halves = cols // LANES
    pitch = wide.shape[2] // ch
    col_odd = lax.axis_index("col") % 2 == 1
    row_odd = lax.axis_index("row") % 2 == 1
    lane = lanes_of((ch, LANES))
    cut = ch // PIECES
    tap_copies = [
        pltpu.make_async_copy(src, dst, tap_sems.at[k])
        for k, (src, dst) in enumerate(((k1, taps1), (k2, taps2)))
    ]
    for copy in tap_copies:
        copy.start()
    copies = []
    for which, ref in enumerate((img, cot)):
        for k in range(PIECES):
            span = pl.ds(k * cut, cut)
            copy = pltpu.make_async_copy(
                ref.at[0, span], staged.at[which, span], sems.at[which, k]
            )
            copy.start()
            copies.append(copy)
    for which in range(2):
        base = which * ch
        left = jnp.zeros((ch, LANES), F32)
        right = jnp.zeros((ch, LANES), F32)
        for k in range(PIECES):
            copies[which * PIECES + k].wait()
            for c in range(k * cut, (k + 1) * cut):
                for half in range(halves):
                    wide[which, half, c * pitch : c * pitch + rows, :] = staged[
                        which, c, :, half * LANES : (half + 1) * LANES
                    ].astype(F32)
        for half in range(halves):
            for h in range(rows):
                v = wide[which, half, pl.ds(h, ch, stride=pitch), :]
                x16[h, base : base + ch, half * LANES : (half + 1) * LANES] = v.astype(BF)
                for j in range(2):
                    at = j * SLOT + h + 2
                    if half == 0:
                        left = jnp.where(lane == at, pltpu.roll(v, (at - j) % LANES, 1), left)
                    if half == halves - 1:
                        src = LANES - 2 + j
                        right = jnp.where(lane == at, pltpu.roll(v, (at - src) % LANES, 1), right)
        own[0, base : base + ch, :] = left.astype(BF)
        own[1, base : base + ch, :] = right.astype(BF)
        send_a[base : base + ch, :] = jnp.where(col_odd, left, right).astype(BF)
        send_b[base : base + ch, :] = jnp.where(col_odd, right, left).astype(BF)
    row_a[...] = x16[pl.ds(jnp.where(row_odd, 0, rows - 2), 2)]
    if row_b is not None:
        row_b[...] = x16[pl.ds(jnp.where(row_odd, rows - 2, 0), 2)]
    for copy in tap_copies:
        copy.wait()


def sides(a, b, odd):
    zero = jnp.zeros(a.shape, a.dtype)
    b = zero if b is None else b
    return jnp.where(odd, a, b), jnp.where(odd, b, a)


def corner_body(rows, strip_a, strip_b, send_a, send_b):
    col_odd = lax.axis_index("col") % 2 == 1
    row_odd = lax.axis_index("row") % 2 == 1
    lane = lanes_of(strip_a.shape)
    west, east = sides(
        strip_a[...].astype(F32), None if strip_b is None else strip_b[...].astype(F32), col_odd
    )
    both = jnp.where(lane < 2 * SLOT, west, pltpu.roll(east, 2 * SLOT, 1))
    slot = lane % SLOT
    down = jnp.where(slot < 2, pltpu.roll(both, (-rows) % LANES, 1), 0.0)
    up = jnp.where((slot >= rows + 2) & (slot < rows + 4), pltpu.roll(both, rows, 1), 0.0)
    send_a[...] = jnp.where(row_odd, up, down).astype(BF)
    if send_b is not None:
        send_b[...] = jnp.where(row_odd, down, up).astype(BF)


def put_shifted(dst, at, half_values, edge, first, last):
    ch = half_values[0].shape[0]
    n = len(half_values)
    fwd = [pltpu.roll(v, 1, 1) for v in half_values]
    back = [pltpu.roll(v, LANES - 1, 1) for v in half_values]
    for k in range(n):
        at_lanes = slice(k * LANES, (k + 1) * LANES)
        before = edge if k == 0 else fwd[k - 1]
        after = edge if k == n - 1 else back[k + 1]
        dst[at, 0:ch, at_lanes] = jnp.where(first, before, fwd[k]).astype(BF)
        dst[at, ch : 2 * ch, at_lanes] = half_values[k].astype(BF)
        dst[at, 2 * ch : 3 * ch, at_lanes] = jnp.where(last, after, back[k]).astype(BF)


def halves_of(v):
    return [v[:, k * LANES : (k + 1) * LANES] for k in range(v.shape[1] // LANES)]


def has_neighbours():
    out = []
    for axis in ("row", "col"):
        at, size = lax.axis_index(axis), lax.axis_size(axis)
        out += [jnp.where(at > 0, 1.0, 0.0), jnp.where(at < size - 1, 1.0, 0.0)]
    return out


def side_strips(strip_a, strip_b):
    return sides(
        strip_a[...].astype(F32),
        None if strip_b is None else strip_b[...].astype(F32),
        lax.axis_index("col") % 2 == 1,
    )


def edge_of(before, behind, lane_before, lane_behind):
    near = lanes_of(before.shape) < LANES // 2
    return jnp.where(
        near,
        pltpu.roll(before, (-lane_before) % LANES, 1),
        pltpu.roll(behind, (LANES - 1 - lane_behind) % LANES, 1),
    )


def border(weights, west, east, left, right):
    e0 = lanes_of(west.shape) < SLOT
    b0 = jnp.where(e0, west, right)
    b1 = jnp.where(e0, pltpu.roll(west, LANES - SLOT, 1), pltpu.roll(east, SLOT, 1))
    b2 = jnp.where(e0, left, east)
    taps = []
    for a in range(3):
        taps += [pltpu.roll(b, (1 - a) % LANES, 1) if a != 1 else b for b in (b0, b1, b2)]
    stack = jnp.concatenate(taps, 0).astype(BF)
    return jnp.dot(weights, stack, preferred_element_type=F32)


def activation(hidden, act_grad):
    s = 0.5 * jnp.tanh(0.5 * hidden) + 0.5
    return hidden * s, act_grad * (s * (1.0 + hidden * (1.0 - s)))


def row_weights(dst, kernel, flip):
    ch = kernel.shape[2]
    zero = jnp.zeros((ch, ch), BF)
    taps = []
    for a in range(3):
        for b in range(3):
            taps.append(kernel[2 - a, 2 - b].T if flip else kernel[a, b])
    for p in range(2):
        blocks = [zero] * (3 * p) + taps + [zero] * (3 - 3 * p)
        for k in range(6):
            dst[p * ch : (p + 1) * ch, k * LANES : (k + 1) * LANES] = jnp.concatenate(
                blocks[2 * k : 2 * k + 2], 1
            )


NT = (((1,), (1,)), ((), ()))


def add_grads(sums, lhs_rows, rhs):
    lhs = jnp.concatenate(lhs_rows, 0)
    return sums + lax.dot_general(lhs, rhs, NT, preferred_element_type=F32)


def inner_body(
    taps1, taps2, x16, own, strip_a, strip_b,
    xi, xc, acts, hids, g1_out, g2_out, wf,
):
    rows, ch2, cols = x16.shape
    ch = ch2 // 2
    row_weights(wf.at[0], taps1, False)
    row_weights(wf.at[1], taps2, True)
    west, east = side_strips(strip_a, strip_b)
    left, right = own[0].astype(F32), own[1].astype(F32)
    first = lanes_of((ch, LANES)) == 0
    last = lanes_of((ch, LANES)) == LANES - 1
    west_b, east_b = west.astype(BF), east.astype(BF)
    for h in range(rows):
        edge = edge_of(west_b, east_b, SLOT + h + 2, h + 2)
        for which, dst in enumerate((xi, xc)):
            s = slice(which * ch, (which + 1) * ch)
            put_shifted(dst, h, halves_of(x16[h, s]), edge[s], first, last)
    lane = lanes_of((ch, LANES))
    _, _, has_west, has_east = has_neighbours()
    keep = jnp.where(lane < SLOT, has_west, has_east) > 0.0
    sides_of = lambda s: (west[s], east[s], left[s], right[s])
    act_e, hid_e = activation(
        border(wf[0, :ch, : 9 * ch], *sides_of(slice(0, ch))),
        border(wf[1, :ch, : 9 * ch], *sides_of(slice(ch, ch2))),
    )
    act_e = jnp.where(keep, act_e, 0.0).astype(BF)
    hid_e = jnp.where(keep, hid_e, 0.0).astype(BF)
    zero_row = jnp.zeros((ch, cols), BF)
    for t in range((rows - 2) // 2):
        at = 2 * t
        hidden = jnp.dot(
            wf[0], xi[at : at + 4].reshape(12 * ch, cols), preferred_element_type=F32
        )
        act_grad = jnp.dot(
            wf[1], xc[at : at + 4].reshape(12 * ch, cols), preferred_element_type=F32
        )
        for values, dst, e in zip(activation(hidden, act_grad), (acts, hids), (act_e, hid_e)):
            for p in range(2):
                h = at + p + 1
                put_shifted(
                    dst, at + p, halves_of(values[p * ch : (p + 1) * ch].astype(BF)),
                    edge_of(e, e, h + 2, SLOT + h + 2), first, last,
                )
    g1 = jnp.zeros((3 * ch, 3 * ch), F32)
    for r in range(rows):
        lhs = [
            hids[h - 1, ch : 2 * ch] if 1 <= h <= rows - 2 else zero_row for h in range(r - 1, r + 2)
        ]
        g1 = add_grads(g1, lhs, xi[r])
    g1_out[...] = g1
    g2 = jnp.zeros((3 * ch, 3 * ch), F32)
    for r in range(1, rows - 1):
        g2 = add_grads(g2, [x16[h, ch:] for h in range(r - 1, r + 2)], acts[r - 1])
    g2_out[...] = g2


def outer_body(
    wf, x16, own, xi, xc, hids, g1_in, g2_in,
    strip_a, strip_b, row_a, row_b, corner_a, corner_b,
    acts_o, hids_o, mine, other, xo, grads,
):
    rows, ch2, cols = x16.shape
    ch = ch2 // 2
    has_north, has_south, has_west, has_east = has_neighbours()
    lane2 = lanes_of((ch2, LANES))
    west, east = side_strips(strip_a, strip_b)
    corner = corner_a[...].astype(F32)
    if corner_b is not None:
        corner = corner + corner_b[...].astype(F32)
    west = west + jnp.where(lane2 < 2 * SLOT, corner, 0.0)
    east = east + jnp.where(lane2 < 2 * SLOT, pltpu.roll(corner, LANES - 2 * SLOT, 1), 0.0)
    north, south = sides(
        row_a[...], None if row_b is None else row_b[...], lax.axis_index("row") % 2 == 1
    )
    left, right = own[0].astype(F32), own[1].astype(F32)
    first = lanes_of((ch, LANES)) == 0
    last = lanes_of((ch, LANES)) == LANES - 1
    west_b, east_b = west.astype(BF), east.astype(BF)
    for k in range(4):
        slot = k if k < 2 else rows + k
        row = (north if k < 2 else south)[k % 2]
        lo, hi = row[:, :LANES].astype(F32), row[:, cols - LANES :].astype(F32)
        left = jnp.where(lane2 == slot, pltpu.roll(lo, slot, 1), left)
        right = jnp.where(
            lane2 == SLOT + slot, pltpu.roll(hi, (SLOT + slot - LANES + 1) % LANES, 1), right
        )
        edge = edge_of(west_b, east_b, SLOT + slot, slot)
        for which in range(2):
            s = slice(which * ch, (which + 1) * ch)
            put_shifted(xo.at[which], k, halves_of(row[s]), edge[s], first, last)
    lane = lanes_of((ch, LANES))
    slots = lane % SLOT
    keep = jnp.where(lane < SLOT, has_west, has_east)
    keep = keep * jnp.where(slots == 1, has_north, 1.0) * jnp.where(slots == rows + 2, has_south, 1.0)
    sides_of = lambda s: (west[s], east[s], left[s], right[s])
    act_e, hid_e = activation(
        border(wf[0, :ch, : 9 * ch], *sides_of(slice(0, ch))),
        border(wf[1, :ch, : 9 * ch], *sides_of(slice(ch, ch2))),
    )
    act_e = jnp.where(keep > 0.0, act_e, 0.0).astype(BF)
    hid_e = jnp.where(keep > 0.0, hid_e, 0.0).astype(BF)
    for t in range(2):
        stacks = []
        for which, mid in enumerate((xi, xc)):
            ends = xo[which, 2 * t : 2 * t + 2].reshape(6 * ch, cols)
            if t == 0:
                stack = [ends, mid[0:2].reshape(6 * ch, cols)]
            else:
                stack = [mid[rows - 2 : rows].reshape(6 * ch, cols), ends]
            stacks.append(jnp.concatenate(stack, 0))
        hidden = jnp.dot(wf[0], stacks[0], preferred_element_type=F32)
        act_grad = jnp.dot(wf[1], stacks[1], preferred_element_type=F32)
        for values, dst, e in zip(activation(hidden, act_grad), (acts_o, hids_o), (act_e, hid_e)):
            for p in range(2):
                at = 2 * t + p
                h = at - 1 if t == 0 else rows - 3 + at
                v = values[p * ch : (p + 1) * ch]
                if at == 0:
                    v = jnp.where(has_north > 0.0, v, 0.0)
                if at == 3:
                    v = jnp.where(has_south > 0.0, v, 0.0)
                put_shifted(
                    dst, at, halves_of(v.astype(BF)), edge_of(e, e, h + 2, SLOT + h + 2), first, last
                )
    zero_row = jnp.zeros((ch, cols), BF)
    g1, g2 = g1_in[...], g2_in[...]
    for k, r in ((0, -1), (1, 0), (2, rows - 1), (3, rows)):
        lhs = [x16[h, ch:] if 0 <= h < rows else zero_row for h in range(r - 1, r + 2)]
        g2 = add_grads(g2, lhs, acts_o[k])
    for h, row in ((0, hids_o[1, ch : 2 * ch]), (rows - 1, hids_o[2, ch : 2 * ch])):
        for r in range(h - 1, h + 2):
            rhs = xi[r] if 0 <= r < rows else xo[0, 1 if r < 0 else 2]
            lhs = [row if h == r - 1 + k else zero_row for k in range(3)]
            g1 = add_grads(g1, lhs, rhs)
    grads[0 : 3 * ch, :] = g1[:, : 2 * ch]
    grads[3 * ch : 6 * ch, :] = g2[:, : 2 * ch]
    grads[6 * ch : 9 * ch, :] = jnp.concatenate([g1[:, 2 * ch :], g2[:, 2 * ch :]], 1)
    count = mine.shape[0]
    core = lax.axis_index("dp") % 2
    mine[...] = grads[pl.ds(core * count, count), :]
    other[...] = grads[pl.ds((1 - core) * count, count), :]


def back_body(flip, kernel, mid, ends, out, weights, wide):
    rows = mid.shape[0] + 2
    ch = kernel.shape[2]
    cols = mid.shape[2]
    pitch = wide.shape[1] // ch
    row_weights(weights, kernel, flip)
    for t in range(rows // 2):
        if t == 0:
            stack = jnp.concatenate([ends[0:2], mid[0:2]], 0)
        elif t == rows // 2 - 1:
            stack = jnp.concatenate([mid[rows - 4 : rows - 2], ends[2:4]], 0)
        else:
            stack = mid[2 * t - 2 : 2 * t + 2]
        y = jnp.dot(weights[...], stack.reshape(12 * ch, cols), preferred_element_type=F32)
        for p in range(2):
            for half, part in enumerate(halves_of(y[p * ch : (p + 1) * ch])):
                wide[half, pl.ds(2 * t + p, ch, stride=pitch), :] = part
    for half in range(cols // LANES):
        for c in range(ch):
            out[0, c, :, half * LANES : (half + 1) * LANES] = wide[
                half, c * pitch : c * pitch + rows, :
            ].astype(BF)


def finish_body(factor, mine, other, first, second):
    core = lax.axis_index("dp") % 2
    m, o = mine[...].astype(F32) * factor, other[...].astype(F32) * factor
    whole = jnp.concatenate([jnp.where(core == 0, m, o), jnp.where(core == 0, o, m)], 0)
    ch = first.shape[2]
    tail = whole[6 * ch :]
    swapped = pltpu.roll(whole, LANES - ch, 1)
    for k, dst in ((0, first), (1, second)):
        for a in range(3):
            src = (2 - a) * ch
            dst[a, 0] = whole[k * 3 * ch + src : k * 3 * ch + src + ch, :ch]
            dst[a, 1] = swapped[k * 3 * ch + src : k * 3 * ch + src + ch, :ch]
            third = tail if k == 0 else swapped[6 * ch :]
            dst[a, 2] = third[src : src + ch, :ch]


def exchange(half, dims):
    axes = ("dp", "row", "col")
    sizes = [lax.axis_size(a) for a in axes]
    sent = half.astype(BF)
    total = sent.astype(F32)
    for pick in range(1, 1 << len(dims)):
        flips = [0, 0, 0]
        for k, (axis, bit) in enumerate(dims):
            if pick >> k & 1:
                flips[axis] ^= bit
        perm = []
        for d in range(sizes[0]):
            for r in range(sizes[1]):
                for c in range(sizes[2]):
                    to = (d ^ flips[0], r ^ flips[1], c ^ flips[2])
                    perm.append(
                        ((d * sizes[1] + r) * sizes[2] + c, (to[0] * sizes[1] + to[1]) * sizes[2] + to[2])
                    )
        total = total + lax.ppermute(sent, axes, perm).astype(F32)
    return total


def on_device(images, first_kernel, second_kernel, cotangent):
    ch, rows, cols = images.shape[1:]
    n_row, n_col, n_dp = (lax.axis_size(a) for a in ("row", "col", "dp"))
    total = rows * cols * n_row * n_col * n_dp * images.shape[0]
    factor = 1.0 / math.sqrt(total)
    pitch = 24
    halves = cols // LANES
    two_rows = n_row > 2
    two_cols = n_col > 2
    sds = jax.ShapeDtypeStruct
    strip = sds((2 * ch, LANES), BF)
    row_pair = sds((2, 2 * ch, cols), BF)
    hbm = pl.BlockSpec(memory_space=pltpu.HBM)

    def optional(body, flags):
        def wrapped(*refs):
            refs = list(refs)
            return body(*[refs.pop(0) if keep else None for keep in flags], *refs)

        return wrapped

    k1 = first_kernel.transpose(2, 3, 0, 1)
    k2 = second_kernel.transpose(2, 3, 0, 1)
    pack = kernel_call(
        optional(pack_body, [True] * 11 + [two_rows]),
        [sds((rows, 2 * ch, cols), BF), sds((2, 2 * ch, LANES), BF)]
        + [sds(k1.shape, BF), sds(k2.shape, BF), strip, strip]
        + [row_pair] * (1 + two_rows),
        [
            pltpu.VMEM((2, ch, rows, cols), BF),
            pltpu.VMEM((2, halves, ch * pitch, LANES), F32),
            pltpu.SemaphoreType.DMA((2, PIECES)),
            pltpu.SemaphoreType.DMA((2,)),
        ],
        in_specs=[hbm] * 4,
        flops=1 << 27,
        name="pack",
    )
    x16, own, taps1, taps2, send_a, send_b, *row_sends = pack(
        *[pltpu.with_memory_space_constraint(v, pltpu.HBM) for v in (images, cotangent, k1, k2)]
    )
    strips = [swap(send_a, "col", False)]
    if two_cols:
        strips.append(swap(send_b, "col", True))
    got_rows = [swap(s, "row", k == 1) for k, s in enumerate(row_sends)]
    corner_sends = kernel_call(
        optional(functools.partial(corner_body, rows), [True, two_cols, True, two_rows]),
        [strip] * (1 + two_rows),
        name="corner",
    )(*strips)
    corners = [swap(s, "row", k == 1) for k, s in enumerate(corner_sends)]
    shifted = lambda n: sds((n, 3 * ch, cols), BF)
    sums = sds((3 * ch, 3 * ch), F32)
    xi, xc, acts, hids, g1, g2, wf = kernel_call(
        optional(inner_body, [True] * 5 + [two_cols]),
        [shifted(rows), shifted(rows), shifted(rows - 2), shifted(rows - 2), sums, sums]
        + [sds((2, 2 * ch, 12 * ch), BF)],
        flops=1 << 30,
        name="inner",
    )(taps1, taps2, x16, own, *strips)
    half = sds((9 * ch // 2, LANES), F32)
    acts_o, hids_o, mine, other = kernel_call(
        optional(outer_body, [True] * 8 + [True, two_cols] + [True, two_rows] * 2),
        [shifted(4), shifted(4), half, half],
        [pltpu.VMEM((2, 4, 3 * ch, cols), BF), pltpu.VMEM((9 * ch, LANES), F32)],
        flops=1 << 28,
        name="outer",
    )(wf, x16, own, xi, xc, hids, g1, g2, *strips, *got_rows, *corners)

    def back(kernel, mid, ends, flip, name):
        return kernel_call(
            functools.partial(back_body, flip),
            [sds(images.shape, BF)],
            [
                pltpu.VMEM((2 * ch, 12 * ch), BF),
                pltpu.VMEM((halves, ch * pitch, LANES), F32),
            ],
            flops=1 << 29,
            name=name,
        )(kernel, mid, ends)[0]

    partner = [(i, i ^ 1) for i in range(n_dp)]
    total_half = mine + lax.ppermute(other, "dp", partner)
    steps = [(0, 1 << k) for k in range(1, n_dp.bit_length() - 1)]
    steps += [(1, 1 << k) for k in range(n_row.bit_length() - 1)]
    steps += [(2, 1 << k) for k in range(n_col.bit_length() - 1)]
    out = back(taps2, acts, acts_o, False, "out")
    grad_in = back(taps1, hids, hids_o, True, "grad_in")
    stages = [steps[k : k + 2] for k in range(0, len(steps), 2)]
    for k, stage in enumerate(stages):
        total_half = exchange(total_half, stage)
        if k == len(stages) - 2:
            total_half, out = lax.optimization_barrier((total_half, out))
        if k == len(stages) - 1:
            total_half, grad_in = lax.optimization_barrier((total_half, grad_in))
    rest = lax.ppermute(total_half, "dp", partner)
    taps = sds((3, 3, ch, ch), F32)
    first, second = kernel_call(
        functools.partial(finish_body, factor), [taps, taps], name="finish"
    )(total_half, rest)
    return out, grad_in, first.transpose(2, 3, 0, 1), second.transpose(2, 3, 0, 1)


def solution(mesh):
    in_specs = (P("dp", None, "row", "col"), P(), P(), P("dp", None, "row", "col"))
    out_specs = (P("dp", None, "row", "col"), P("dp", None, "row", "col"), P(), P())
    return jax.shard_map(
        on_device, mesh=mesh, in_specs=in_specs, out_specs=out_specs, check_vma=False
    )
```

```python
import functools
import math

import jax
import jax.numpy as jnp
from jax import lax
from jax.experimental import pallas as pl
from jax.experimental.pallas import tpu as pltpu
from jax.sharding import PartitionSpec as P

BF = jnp.bfloat16
F32 = jnp.float32
LANES = 128
SLOT = 32
PIECES = 2


def kernel_call(body, outs, scratch=(), flops=0, name=None, **more):
    return pl.pallas_call(
        body,
        out_shape=outs,
        **more,
        scratch_shapes=list(scratch),
        cost_estimate=pl.CostEstimate(flops=flops, transcendentals=0, bytes_accessed=1 << 20),
        compiler_params=pltpu.CompilerParams(vmem_limit_bytes=24 << 20),
        name=name,
    )


def lanes_of(shape):
    return lax.broadcasted_iota(jnp.int32, shape, len(shape) - 1)


def pairs(size, second):
    out = list(range(size))
    for i in range(1 if second else 0, size - 1, 2):
        out[i], out[i + 1] = i + 1, i
    return out


def swap(array, axis, second):
    size, n_dp = lax.axis_size(axis), lax.axis_size("dp")
    partner = pairs(size, second)
    if partner == list(range(size)):
        return None
    lone = lambda d: d ^ 1 if (d | 1) < n_dp else d
    perm = []
    for d in range(n_dp):
        for i, to in enumerate(partner):
            perm.append((d * size + i, (lone(d) if to == i else d) * size + to))
    return lax.ppermute(array, ("dp", axis), perm)


def pack_body(
    img, cot, k1, k2, x16, own, taps1, taps2, send_a, send_b, row_a, row_b,
    staged, wide, sems, tap_sems,
):
    ch, rows, cols = img.shape[1:]
    halves = cols // LANES
    pitch = wide.shape[2] // (ch + 1)
    col_odd = lax.axis_index("col") % 2 == 1
    row_odd = lax.axis_index("row") % 2 == 1
    lane = lanes_of((ch, LANES))
    cut = ch // PIECES
    tap_copies = [
        pltpu.make_async_copy(src, dst, tap_sems.at[k])
        for k, (src, dst) in enumerate(((k1, taps1), (k2, taps2)))
    ]
    for copy in tap_copies:
        copy.start()
    copies = []
    for which, ref in enumerate((img, cot)):
        for k in range(PIECES):
            span = pl.ds(k * cut, cut)
            copy = pltpu.make_async_copy(
                ref.at[0, span], staged.at[which, span], sems.at[which, k]
            )
            copy.start()
            copies.append(copy)
    for which in range(2):
        base = which * ch
        left = jnp.zeros((ch, LANES), F32)
        right = jnp.zeros((ch, LANES), F32)
        for k in range(PIECES):
            copies[which * PIECES + k].wait()
            for c in range(k * cut, (k + 1) * cut):
                for half in range(halves):
                    wide[which, half, c * pitch : c * pitch + rows, :] = staged[
                        which, c, :, half * LANES : (half + 1) * LANES
                    ].astype(F32)
        for half in range(halves):
            for h in range(rows):
                v = wide[which, half, pl.ds(h, ch, stride=pitch), :]
                x16[h, base : base + ch, half * LANES : (half + 1) * LANES] = v.astype(BF)
                for j in range(2):
                    at = j * SLOT + h + 2
                    if half == 0:
                        left = jnp.where(lane == at, pltpu.roll(v, (at - j) % LANES, 1), left)
                    if half == halves - 1:
                        src = LANES - 2 + j
                        right = jnp.where(lane == at, pltpu.roll(v, (at - src) % LANES, 1), right)
        own[0, base : base + ch, :] = left.astype(BF)
        own[1, base : base + ch, :] = right.astype(BF)
        send_a[base : base + ch, :] = jnp.where(col_odd, left, right).astype(BF)
        send_b[base : base + ch, :] = jnp.where(col_odd, right, left).astype(BF)
    row_a[...] = x16[pl.ds(jnp.where(row_odd, 0, rows - 2), 2)]
    if row_b is not None:
        row_b[...] = x16[pl.ds(jnp.where(row_odd, rows - 2, 0), 2)]
    for copy in tap_copies:
        copy.wait()


def sides(a, b, axis):
    at, size = lax.axis_index(axis), lax.axis_size(axis)
    b = a if b is None else b
    odd = at % 2 == 1
    zero = jnp.zeros(a.shape, a.dtype)
    before = jnp.where(at > 0, jnp.where(odd, a, b), zero)
    behind = jnp.where(at < size - 1, jnp.where(odd, b, a), zero)
    return before, behind


def corner_body(rows, strip_a, strip_b, send_a, send_b):
    row_odd = lax.axis_index("row") % 2 == 1
    lane = lanes_of(strip_a.shape)
    west, east = side_strips(strip_a, strip_b)
    both = jnp.where(lane < 2 * SLOT, west, pltpu.roll(east, 2 * SLOT, 1))
    slot = lane % SLOT
    down = jnp.where(slot < 2, pltpu.roll(both, (-rows) % LANES, 1), 0.0)
    up = jnp.where((slot >= rows + 2) & (slot < rows + 4), pltpu.roll(both, rows, 1), 0.0)
    send_a[...] = jnp.where(row_odd, up, down).astype(BF)
    if send_b is not None:
        send_b[...] = jnp.where(row_odd, down, up).astype(BF)


def put_shifted(dst, at, half_values, edge, first, last):
    ch = half_values[0].shape[0]
    n = len(half_values)
    fwd = [pltpu.roll(v, 1, 1) for v in half_values]
    back = [pltpu.roll(v, LANES - 1, 1) for v in half_values]
    for k in range(n):
        at_lanes = slice(k * LANES, (k + 1) * LANES)
        before = edge if k == 0 else fwd[k - 1]
        after = edge if k == n - 1 else back[k + 1]
        dst[at, 0:ch, at_lanes] = jnp.where(first, before, fwd[k]).astype(BF)
        dst[at, ch : 2 * ch, at_lanes] = half_values[k].astype(BF)
        dst[at, 2 * ch : 3 * ch, at_lanes] = jnp.where(last, after, back[k]).astype(BF)


def halves_of(v):
    return [v[:, k * LANES : (k + 1) * LANES] for k in range(v.shape[1] // LANES)]


def has_neighbours():
    out = []
    for axis in ("row", "col"):
        at, size = lax.axis_index(axis), lax.axis_size(axis)
        out += [jnp.where(at > 0, 1.0, 0.0), jnp.where(at < size - 1, 1.0, 0.0)]
    return out


def side_strips(strip_a, strip_b):
    return sides(
        strip_a[...].astype(F32),
        None if strip_b is None else strip_b[...].astype(F32),
        "col",
    )


def edge_of(before, behind, lane_before, lane_behind):
    near = lanes_of(before.shape) < LANES // 2
    return jnp.where(
        near,
        pltpu.roll(before, (-lane_before) % LANES, 1),
        pltpu.roll(behind, (LANES - 1 - lane_behind) % LANES, 1),
    )


def border(weights, west, east, left, right):
    e0 = lanes_of(west.shape) < SLOT
    b0 = jnp.where(e0, west, right)
    b1 = jnp.where(e0, pltpu.roll(west, LANES - SLOT, 1), pltpu.roll(east, SLOT, 1))
    b2 = jnp.where(e0, left, east)
    taps = []
    for a in range(3):
        taps += [pltpu.roll(b, (1 - a) % LANES, 1) if a != 1 else b for b in (b0, b1, b2)]
    stack = jnp.concatenate(taps, 0).astype(BF)
    return jnp.dot(weights, stack, preferred_element_type=F32)


def activation(hidden, act_grad):
    s = 0.5 * jnp.tanh(0.5 * hidden) + 0.5
    return hidden * s, act_grad * (s * (1.0 + hidden * (1.0 - s)))


def row_weights(dst, kernel, flip):
    ch = kernel.shape[2]
    zero = jnp.zeros((ch, ch), BF)
    taps = []
    for a in range(3):
        for b in range(3):
            taps.append(kernel[2 - a, 2 - b].T if flip else kernel[a, b])
    for p in range(2):
        blocks = [zero] * (3 * p) + taps + [zero] * (3 - 3 * p)
        for k in range(6):
            dst[p * ch : (p + 1) * ch, k * LANES : (k + 1) * LANES] = jnp.concatenate(
                blocks[2 * k : 2 * k + 2], 1
            )


NT = (((1,), (1,)), ((), ()))


def add_grads(sums, lhs_rows, rhs):
    lhs = jnp.concatenate(lhs_rows, 0)
    return sums + lax.dot_general(lhs, rhs, NT, preferred_element_type=F32)


def inner_body(
    taps1, taps2, x16, own, strip_a, strip_b,
    xi, xc, acts, hids, g1_out, g2_out, wf,
):
    rows, ch2, cols = x16.shape
    ch = ch2 // 2
    row_weights(wf.at[0], taps1, False)
    row_weights(wf.at[1], taps2, True)
    west, east = side_strips(strip_a, strip_b)
    left, right = own[0].astype(F32), own[1].astype(F32)
    first = lanes_of((ch, LANES)) == 0
    last = lanes_of((ch, LANES)) == LANES - 1
    west_b, east_b = west.astype(BF), east.astype(BF)
    for h in range(rows):
        edge = edge_of(west_b, east_b, SLOT + h + 2, h + 2)
        for which, dst in enumerate((xi, xc)):
            s = slice(which * ch, (which + 1) * ch)
            put_shifted(dst, h, halves_of(x16[h, s]), edge[s], first, last)
    lane = lanes_of((ch, LANES))
    _, _, has_west, has_east = has_neighbours()
    keep = jnp.where(lane < SLOT, has_west, has_east) > 0.0
    sides_of = lambda s: (west[s], east[s], left[s], right[s])
    act_e, hid_e = activation(
        border(wf[0, :ch, : 9 * ch], *sides_of(slice(0, ch))),
        border(wf[1, :ch, : 9 * ch], *sides_of(slice(ch, ch2))),
    )
    act_e = jnp.where(keep, act_e, 0.0).astype(BF)
    hid_e = jnp.where(keep, hid_e, 0.0).astype(BF)
    zero_row = jnp.zeros((ch, cols), BF)
    for t in range((rows - 2) // 2):
        at = 2 * t
        hidden = jnp.dot(
            wf[0], xi[at : at + 4].reshape(12 * ch, cols), preferred_element_type=F32
        )
        act_grad = jnp.dot(
            wf[1], xc[at : at + 4].reshape(12 * ch, cols), preferred_element_type=F32
        )
        for values, dst, e in zip(activation(hidden, act_grad), (acts, hids), (act_e, hid_e)):
            for p in range(2):
                h = at + p + 1
                put_shifted(
                    dst, at + p, halves_of(values[p * ch : (p + 1) * ch].astype(BF)),
                    edge_of(e, e, h + 2, SLOT + h + 2), first, last,
                )
    g1 = jnp.zeros((3 * ch, 3 * ch), F32)
    for r in range(rows):
        lhs = [
            hids[h - 1, ch : 2 * ch] if 1 <= h <= rows - 2 else zero_row for h in range(r - 1, r + 2)
        ]
        g1 = add_grads(g1, lhs, xi[r])
    g1_out[...] = g1
    g2 = jnp.zeros((3 * ch, 3 * ch), F32)
    for r in range(1, rows - 1):
        g2 = add_grads(g2, [x16[h, ch:] for h in range(r - 1, r + 2)], acts[r - 1])
    g2_out[...] = g2


def outer_body(
    wf, x16, own, xi, xc, hids, g1_in, g2_in,
    strip_a, strip_b, row_a, row_b, corner_a, corner_b,
    acts_o, hids_o, mine, other, xo, grads,
):
    rows, ch2, cols = x16.shape
    ch = ch2 // 2
    has_north, has_south, has_west, has_east = has_neighbours()
    west, east = side_strips(strip_a, strip_b)
    lane2 = lanes_of((ch2, LANES))
    above, below = sides(
        corner_a[...].astype(F32), None if corner_b is None else corner_b[...].astype(F32), "row"
    )
    corner = jnp.where(lane2 % SLOT < 2, above, below)
    west = west + jnp.where(lane2 < 2 * SLOT, corner, 0.0)
    east = east + jnp.where(lane2 < 2 * SLOT, pltpu.roll(corner, LANES - 2 * SLOT, 1), 0.0)
    north, south = sides(row_a[...], None if row_b is None else row_b[...], "row")
    left, right = own[0].astype(F32), own[1].astype(F32)
    first = lanes_of((ch, LANES)) == 0
    last = lanes_of((ch, LANES)) == LANES - 1
    west_b, east_b = west.astype(BF), east.astype(BF)
    for k in range(4):
        slot = k if k < 2 else rows + k
        row = (north if k < 2 else south)[k % 2]
        lo, hi = row[:, :LANES].astype(F32), row[:, cols - LANES :].astype(F32)
        left = jnp.where(lane2 == slot, pltpu.roll(lo, slot, 1), left)
        right = jnp.where(
            lane2 == SLOT + slot, pltpu.roll(hi, (SLOT + slot - LANES + 1) % LANES, 1), right
        )
        edge = edge_of(west_b, east_b, SLOT + slot, slot)
        for which in range(2):
            s = slice(which * ch, (which + 1) * ch)
            put_shifted(xo.at[which], k, halves_of(row[s]), edge[s], first, last)
    lane = lanes_of((ch, LANES))
    slots = lane % SLOT
    keep = jnp.where(lane < SLOT, has_west, has_east)
    keep = keep * jnp.where(slots == 1, has_north, 1.0) * jnp.where(slots == rows + 2, has_south, 1.0)
    sides_of = lambda s: (west[s], east[s], left[s], right[s])
    act_e, hid_e = activation(
        border(wf[0, :ch, : 9 * ch], *sides_of(slice(0, ch))),
        border(wf[1, :ch, : 9 * ch], *sides_of(slice(ch, ch2))),
    )
    act_e = jnp.where(keep > 0.0, act_e, 0.0).astype(BF)
    hid_e = jnp.where(keep > 0.0, hid_e, 0.0).astype(BF)
    for t in range(2):
        stacks = []
        for which, mid in enumerate((xi, xc)):
            ends = xo[which, 2 * t : 2 * t + 2].reshape(6 * ch, cols)
            if t == 0:
                stack = [ends, mid[0:2].reshape(6 * ch, cols)]
            else:
                stack = [mid[rows - 2 : rows].reshape(6 * ch, cols), ends]
            stacks.append(jnp.concatenate(stack, 0))
        hidden = jnp.dot(wf[0], stacks[0], preferred_element_type=F32)
        act_grad = jnp.dot(wf[1], stacks[1], preferred_element_type=F32)
        for values, dst, e in zip(activation(hidden, act_grad), (acts_o, hids_o), (act_e, hid_e)):
            for p in range(2):
                at = 2 * t + p
                h = at - 1 if t == 0 else rows - 3 + at
                v = values[p * ch : (p + 1) * ch]
                if at == 0:
                    v = jnp.where(has_north > 0.0, v, 0.0)
                if at == 3:
                    v = jnp.where(has_south > 0.0, v, 0.0)
                put_shifted(
                    dst, at, halves_of(v.astype(BF)), edge_of(e, e, h + 2, SLOT + h + 2), first, last
                )
    zero_row = jnp.zeros((ch, cols), BF)
    g1, g2 = g1_in[...], g2_in[...]
    for k, r in ((0, -1), (1, 0), (2, rows - 1), (3, rows)):
        lhs = [x16[h, ch:] if 0 <= h < rows else zero_row for h in range(r - 1, r + 2)]
        g2 = add_grads(g2, lhs, acts_o[k])
    for h, row in ((0, hids_o[1, ch : 2 * ch]), (rows - 1, hids_o[2, ch : 2 * ch])):
        for r in range(h - 1, h + 2):
            rhs = xi[r] if 0 <= r < rows else xo[0, 1 if r < 0 else 2]
            lhs = [row if h == r - 1 + k else zero_row for k in range(3)]
            g1 = add_grads(g1, lhs, rhs)
    grads[0 : 3 * ch, :] = g1[:, : 2 * ch]
    grads[3 * ch : 6 * ch, :] = g2[:, : 2 * ch]
    grads[6 * ch : 9 * ch, :] = jnp.concatenate([g1[:, 2 * ch :], g2[:, 2 * ch :]], 1)
    count = mine.shape[0]
    core = lax.axis_index("dp") % 2
    mine[...] = grads[pl.ds(core * count, count), :]
    other[...] = grads[pl.ds((1 - core) * count, count), :]


def back_body(flip, kernel, mid, ends, out, weights, wide):
    rows = mid.shape[0] + 2
    ch = kernel.shape[2]
    cols = mid.shape[2]
    pitch = wide.shape[1] // (ch + 1)
    row_weights(weights, kernel, flip)
    for t in range(rows // 2):
        if t == 0:
            stack = jnp.concatenate([ends[0:2], mid[0:2]], 0)
        elif t == rows // 2 - 1:
            stack = jnp.concatenate([mid[rows - 4 : rows - 2], ends[2:4]], 0)
        else:
            stack = mid[2 * t - 2 : 2 * t + 2]
        y = jnp.dot(weights[...], stack.reshape(12 * ch, cols), preferred_element_type=F32)
        for p in range(2):
            for half, part in enumerate(halves_of(y[p * ch : (p + 1) * ch])):
                wide[half, pl.ds(2 * t + p, ch, stride=pitch), :] = part
    for half in range(cols // LANES):
        for c in range(ch):
            out[0, c, :, half * LANES : (half + 1) * LANES] = wide[
                half, c * pitch : c * pitch + rows, :
            ].astype(BF)


def finish_body(factor, mine, other, first, second):
    core = lax.axis_index("dp") % 2
    m, o = mine[...].astype(F32) * factor, other[...].astype(F32) * factor
    whole = jnp.concatenate([jnp.where(core == 0, m, o), jnp.where(core == 0, o, m)], 0)
    ch = first.shape[2]
    tail = whole[6 * ch :]
    swapped = pltpu.roll(whole, LANES - ch, 1)
    for k, dst in ((0, first), (1, second)):
        for a in range(3):
            src = (2 - a) * ch
            dst[a, 0] = whole[k * 3 * ch + src : k * 3 * ch + src + ch, :ch]
            dst[a, 1] = swapped[k * 3 * ch + src : k * 3 * ch + src + ch, :ch]
            third = tail if k == 0 else swapped[6 * ch :]
            dst[a, 2] = third[src : src + ch, :ch]


def exchange(half, dims):
    axes = ("dp", "row", "col")
    sizes = [lax.axis_size(a) for a in axes]
    sent = half.astype(BF)
    total = sent.astype(F32)
    for pick in range(1, 1 << len(dims)):
        flips = [0, 0, 0]
        for k, (axis, bit) in enumerate(dims):
            if pick >> k & 1:
                flips[axis] ^= bit
        perm = []
        for d in range(sizes[0]):
            for r in range(sizes[1]):
                for c in range(sizes[2]):
                    to = (d ^ flips[0], r ^ flips[1], c ^ flips[2])
                    perm.append(
                        ((d * sizes[1] + r) * sizes[2] + c, (to[0] * sizes[1] + to[1]) * sizes[2] + to[2])
                    )
        total = total + lax.ppermute(sent, axes, perm).astype(F32)
    return total


def on_device(images, first_kernel, second_kernel, cotangent):
    ch, rows, cols = images.shape[1:]
    n_row, n_col, n_dp = (lax.axis_size(a) for a in ("row", "col", "dp"))
    total = rows * cols * n_row * n_col * n_dp * images.shape[0]
    factor = 1.0 / math.sqrt(total)
    pitch = 24
    halves = cols // LANES
    two_rows = n_row > 2
    two_cols = n_col > 2
    sds = jax.ShapeDtypeStruct
    strip = sds((2 * ch, LANES), BF)
    row_pair = sds((2, 2 * ch, cols), BF)
    hbm = pl.BlockSpec(memory_space=pltpu.HBM)

    def optional(body, flags):
        def wrapped(*refs):
            refs = list(refs)
            return body(*[refs.pop(0) if keep else None for keep in flags], *refs)

        return wrapped

    k1 = first_kernel.transpose(2, 3, 0, 1)
    k2 = second_kernel.transpose(2, 3, 0, 1)
    pack = kernel_call(
        optional(pack_body, [True] * 11 + [two_rows]),
        [sds((rows, 2 * ch, cols), BF), sds((2, 2 * ch, LANES), BF)]
        + [sds(k1.shape, BF), sds(k2.shape, BF), strip, strip]
        + [row_pair] * (1 + two_rows),
        [
            pltpu.VMEM((2, ch, rows, cols), BF),
            pltpu.VMEM((2, halves, (ch + 1) * pitch, LANES), F32),
            pltpu.SemaphoreType.DMA((2, PIECES)),
            pltpu.SemaphoreType.DMA((2,)),
        ],
        in_specs=[hbm] * 4,
        flops=1 << 27,
        name="pack",
    )
    x16, own, taps1, taps2, send_a, send_b, *row_sends = pack(
        *[pltpu.with_memory_space_constraint(v, pltpu.HBM) for v in (images, cotangent, k1, k2)]
    )
    strips = [swap(send_a, "col", False)]
    if two_cols:
        strips.append(swap(send_b, "col", True))
    got_rows = [swap(s, "row", k == 1) for k, s in enumerate(row_sends)]
    corner_sends = kernel_call(
        optional(functools.partial(corner_body, rows), [True, two_cols, True, two_rows]),
        [strip] * (1 + two_rows),
        name="corner",
    )(*strips)
    corners = [swap(s, "row", k == 1) for k, s in enumerate(corner_sends)]
    shifted = lambda n: sds((n, 3 * ch, cols), BF)
    sums = sds((3 * ch, 3 * ch), F32)
    xi, xc, acts, hids, g1, g2, wf = kernel_call(
        optional(inner_body, [True] * 5 + [two_cols]),
        [shifted(rows), shifted(rows), shifted(rows - 2), shifted(rows - 2), sums, sums]
        + [sds((2, 2 * ch, 12 * ch), BF)],
        flops=1 << 30,
        name="inner",
    )(taps1, taps2, x16, own, *strips)
    half = sds((9 * ch // 2, LANES), F32)
    acts_o, hids_o, mine, other = kernel_call(
        optional(outer_body, [True] * 8 + [True, two_cols] + [True, two_rows] * 2),
        [shifted(4), shifted(4), half, half],
        [pltpu.VMEM((2, 4, 3 * ch, cols), BF), pltpu.VMEM((9 * ch, LANES), F32)],
        flops=1 << 28,
        name="outer",
    )(wf, x16, own, xi, xc, hids, g1, g2, *strips, *got_rows, *corners)

    def back(kernel, mid, ends, flip, name):
        return kernel_call(
            functools.partial(back_body, flip),
            [sds(images.shape, BF)],
            [
                pltpu.VMEM((2 * ch, 12 * ch), BF),
                pltpu.VMEM((halves, (ch + 1) * pitch, LANES), F32),
            ],
            flops=1 << 29,
            name=name,
        )(kernel, mid, ends)[0]

    partner = [(i, i ^ 1) for i in range(n_dp)]
    total_half = mine + lax.ppermute(other, "dp", partner)
    steps = [(0, 1 << k) for k in range(1, n_dp.bit_length() - 1)]
    steps += [(1, 1 << k) for k in range(n_row.bit_length() - 1)]
    steps += [(2, 1 << k) for k in range(n_col.bit_length() - 1)]
    out = back(taps2, acts, acts_o, False, "out")
    grad_in = back(taps1, hids, hids_o, True, "grad_in")
    stages = [steps[k : k + 2] for k in range(0, len(steps), 2)]
    for k, stage in enumerate(stages):
        total_half = exchange(total_half, stage)
        if k == len(stages) - 2:
            total_half, out = lax.optimization_barrier((total_half, out))
        if k == len(stages) - 1:
            total_half, grad_in = lax.optimization_barrier((total_half, grad_in))
    rest = lax.ppermute(total_half, "dp", partner)
    taps = sds((3, 3, ch, ch), F32)
    first, second = kernel_call(
        functools.partial(finish_body, factor), [taps, taps], name="finish"
    )(total_half, rest)
    return out, grad_in, first.transpose(2, 3, 0, 1), second.transpose(2, 3, 0, 1)


def solution(mesh):
    in_specs = (P("dp", None, "row", "col"), P(), P(), P("dp", None, "row", "col"))
    out_specs = (P("dp", None, "row", "col"), P("dp", None, "row", "col"), P(), P())
    return jax.shard_map(
        on_device, mesh=mesh, in_specs=in_specs, out_specs=out_specs, check_vma=False
    )
```

```python
import functools
import math

import jax
import jax.numpy as jnp
from jax import lax
from jax.experimental import pallas as pl
from jax.experimental.pallas import tpu as pltpu
from jax.sharding import PartitionSpec as P

BF = jnp.bfloat16
F32 = jnp.float32
LANES = 128
SLOT = LANES // 2
PIECES = 2


def kernel_call(body, outs, scratch=(), flops=0, name=None, **more):
    return pl.pallas_call(
        body,
        out_shape=outs,
        **more,
        scratch_shapes=list(scratch),
        cost_estimate=pl.CostEstimate(flops=flops, transcendentals=0, bytes_accessed=1 << 20),
        compiler_params=pltpu.CompilerParams(vmem_limit_bytes=24 << 20),
        name=name,
    )


def lanes_of(shape):
    return lax.broadcasted_iota(jnp.int32, shape, len(shape) - 1)


def pairs(size, second):
    out = list(range(size))
    for i in range(1 if second else 0, size - 1, 2):
        out[i], out[i + 1] = i + 1, i
    return out


def swap(array, axis, second):
    size, n_dp = lax.axis_size(axis), lax.axis_size("dp")
    partner = pairs(size, second)
    if partner == list(range(size)):
        return None
    lone = lambda d: d ^ 1 if (d | 1) < n_dp else d
    perm = []
    for d in range(n_dp):
        for i, to in enumerate(partner):
            perm.append((d * size + i, (lone(d) if to == i else d) * size + to))
    return lax.ppermute(array, ("dp", axis), perm)


def pack_body(
    img, cot, k1, k2, x16, own, taps1, taps2, send_a, send_b, row_a, row_b,
    staged, wide, sems, tap_sems,
):
    ch, rows, cols = img.shape[1:]
    halves = cols // LANES
    pitch = wide.shape[2] // (ch + 1)
    col_odd = lax.axis_index("col") % 2 == 1
    row_odd = lax.axis_index("row") % 2 == 1
    lane = lanes_of((ch, LANES))
    cut = ch // PIECES
    tap_copies = [
        pltpu.make_async_copy(src, dst, tap_sems.at[k])
        for k, (src, dst) in enumerate(((k1, taps1), (k2, taps2)))
    ]
    for copy in tap_copies:
        copy.start()
    copies = []
    for which, ref in enumerate((img, cot)):
        for k in range(PIECES):
            span = pl.ds(k * cut, cut)
            copy = pltpu.make_async_copy(
                ref.at[0, span], staged.at[which, span], sems.at[which, k]
            )
            copy.start()
            copies.append(copy)
    for which in range(2):
        base = which * ch
        left = jnp.zeros((ch, LANES), F32)
        right = jnp.zeros((ch, LANES), F32)
        for k in range(PIECES):
            copies[which * PIECES + k].wait()
            for c in range(k * cut, (k + 1) * cut):
                for half in range(halves):
                    wide[which, half, c * pitch : c * pitch + rows, :] = staged[
                        which, c, :, half * LANES : (half + 1) * LANES
                    ].astype(F32)
        for half in range(halves):
            for h in range(rows):
                v = wide[which, half, pl.ds(h, ch, stride=pitch), :]
                x16[h, base : base + ch, half * LANES : (half + 1) * LANES] = v.astype(BF)
                at = 2 * (h + 2)
                here = (lane >= at) & (lane < at + 2)
                if half == 0:
                    left = jnp.where(here, pltpu.roll(v, at, 1), left)
                if half == halves - 1:
                    right = jnp.where(here, pltpu.roll(v, (at + 2) % LANES, 1), right)
        own[0, base : base + ch, :] = left.astype(BF)
        own[1, base : base + ch, :] = right.astype(BF)
        send_a[base : base + ch, :] = jnp.where(col_odd, left, right).astype(BF)
        send_b[base : base + ch, :] = jnp.where(col_odd, right, left).astype(BF)
    row_a[...] = x16[pl.ds(jnp.where(row_odd, 0, rows - 2), 2)]
    if row_b is not None:
        row_b[...] = x16[pl.ds(jnp.where(row_odd, rows - 2, 0), 2)]
    for copy in tap_copies:
        copy.wait()


def sides(a, b, axis):
    at, size = lax.axis_index(axis), lax.axis_size(axis)
    b = a if b is None else b
    odd = at % 2 == 1
    zero = jnp.zeros(a.shape, a.dtype)
    before = jnp.where(at > 0, jnp.where(odd, a, b), zero)
    behind = jnp.where(at < size - 1, jnp.where(odd, b, a), zero)
    return before, behind


def corner_body(rows, strip_a, strip_b, send_a, send_b):
    row_odd = lax.axis_index("row") % 2 == 1
    lane = lanes_of(strip_a.shape)
    west, east = side_strips(strip_a, strip_b)
    both = jnp.where(lane < SLOT, west, pltpu.roll(east, SLOT, 1))
    slot = lane % SLOT
    down = jnp.where(slot < 4, pltpu.roll(both, (-2 * rows) % LANES, 1), 0.0)
    far = (slot >= 2 * (rows + 2)) & (slot < 2 * (rows + 4))
    up = jnp.where(far, pltpu.roll(both, (2 * rows) % LANES, 1), 0.0)
    send_a[...] = jnp.where(row_odd, up, down).astype(BF)
    if send_b is not None:
        send_b[...] = jnp.where(row_odd, down, up).astype(BF)


def put_shifted(dst, at, half_values, edge, first, last):
    ch = half_values[0].shape[0]
    n = len(half_values)
    fwd = [pltpu.roll(v, 1, 1) for v in half_values]
    back = [pltpu.roll(v, LANES - 1, 1) for v in half_values]
    for k in range(n):
        at_lanes = slice(k * LANES, (k + 1) * LANES)
        before = edge if k == 0 else fwd[k - 1]
        after = edge if k == n - 1 else back[k + 1]
        dst[at, 0:ch, at_lanes] = jnp.where(first, before, fwd[k]).astype(BF)
        dst[at, ch : 2 * ch, at_lanes] = half_values[k].astype(BF)
        dst[at, 2 * ch : 3 * ch, at_lanes] = jnp.where(last, after, back[k]).astype(BF)


def halves_of(v):
    return [v[:, k * LANES : (k + 1) * LANES] for k in range(v.shape[1] // LANES)]


def has_neighbours():
    out = []
    for axis in ("row", "col"):
        at, size = lax.axis_index(axis), lax.axis_size(axis)
        out += [jnp.where(at > 0, 1.0, 0.0), jnp.where(at < size - 1, 1.0, 0.0)]
    return out


def side_strips(strip_a, strip_b):
    return sides(
        strip_a[...].astype(F32),
        None if strip_b is None else strip_b[...].astype(F32),
        "col",
    )


def even_lanes(shape):
    return lanes_of(shape) % 2 == 0


def edge_of(strips, h):
    return pltpu.roll(strips, (-2 * (h + 2) - 1) % LANES, 1)


def border(weights, west, east, left, right):
    even = even_lanes(west.shape)
    b0 = jnp.where(even, west, right)
    b1 = jnp.where(even, pltpu.roll(west, LANES - 1, 1), pltpu.roll(east, 1, 1))
    b2 = jnp.where(even, left, east)
    taps = []
    for a in range(3):
        taps += [pltpu.roll(b, (2 - 2 * a) % LANES, 1) if a != 1 else b for b in (b0, b1, b2)]
    stack = jnp.concatenate(taps, 0).astype(BF)
    return jnp.dot(weights, stack, preferred_element_type=F32)


def crossed(strips):
    v = strips.astype(BF)
    return jnp.where(even_lanes(v.shape), pltpu.roll(v, LANES - 1, 1), pltpu.roll(v, 1, 1))


def activation(hidden, act_grad):
    s = 0.5 * jnp.tanh(0.5 * hidden) + 0.5
    return hidden * s, act_grad * (s * (1.0 + hidden * (1.0 - s)))


def row_weights(dst, kernel, flip):
    ch = kernel.shape[2]
    zero = jnp.zeros((ch, ch), BF)
    taps = []
    for a in range(3):
        for b in range(3):
            taps.append(kernel[2 - a, 2 - b].T if flip else kernel[a, b])
    for p in range(2):
        blocks = [zero] * (3 * p) + taps + [zero] * (3 - 3 * p)
        for k in range(6):
            dst[p * ch : (p + 1) * ch, k * LANES : (k + 1) * LANES] = jnp.concatenate(
                blocks[2 * k : 2 * k + 2], 1
            )


NT = (((1,), (1,)), ((), ()))


def add_grads(sums, lhs_rows, rhs):
    lhs = jnp.concatenate(lhs_rows, 0)
    return sums + lax.dot_general(lhs, rhs, NT, preferred_element_type=F32)


def inner_body(
    taps1, taps2, x16, own, strip_a, strip_b,
    xi, xc, acts, hids, g1_out, g2_out, wf,
):
    rows, ch2, cols = x16.shape
    ch = ch2 // 2
    row_weights(wf.at[0], taps1, False)
    row_weights(wf.at[1], taps2, True)
    west, east = side_strips(strip_a, strip_b)
    left, right = own[0].astype(F32), own[1].astype(F32)
    first = lanes_of((ch, LANES)) == 0
    last = lanes_of((ch, LANES)) == LANES - 1
    near = jnp.where(even_lanes(west.shape), east, west).astype(BF)
    for h in range(rows):
        edge = edge_of(near, h)
        for which, dst in enumerate((xi, xc)):
            s = slice(which * ch, (which + 1) * ch)
            put_shifted(dst, h, halves_of(x16[h, s]), edge[s], first, last)
    lane = lanes_of((ch, LANES))
    _, _, has_west, has_east = has_neighbours()
    keep = jnp.where(lane % 2 == 0, has_west, has_east) > 0.0
    sides_of = lambda s: (west[s], east[s], left[s], right[s])
    act_e, hid_e = activation(
        border(wf[0, :ch, : 9 * ch], *sides_of(slice(0, ch))),
        border(wf[1, :ch, : 9 * ch], *sides_of(slice(ch, ch2))),
    )
    act_e = crossed(jnp.where(keep, act_e, 0.0))
    hid_e = crossed(jnp.where(keep, hid_e, 0.0))
    zero_row = jnp.zeros((ch, cols), BF)
    for t in range((rows - 2) // 2):
        at = 2 * t
        hidden = jnp.dot(
            wf[0], xi[at : at + 4].reshape(12 * ch, cols), preferred_element_type=F32
        )
        act_grad = jnp.dot(
            wf[1], xc[at : at + 4].reshape(12 * ch, cols), preferred_element_type=F32
        )
        for values, dst, e in zip(activation(hidden, act_grad), (acts, hids), (act_e, hid_e)):
            for p in range(2):
                h = at + p + 1
                put_shifted(
                    dst, at + p, halves_of(values[p * ch : (p + 1) * ch].astype(BF)),
                    edge_of(e, h), first, last,
                )
    g1 = jnp.zeros((3 * ch, 3 * ch), F32)
    for r in range(rows):
        lhs = [
            hids[h - 1, ch : 2 * ch] if 1 <= h <= rows - 2 else zero_row for h in range(r - 1, r + 2)
        ]
        g1 = add_grads(g1, lhs, xi[r])
    g1_out[...] = g1
    g2 = jnp.zeros((3 * ch, 3 * ch), F32)
    for r in range(1, rows - 1):
        g2 = add_grads(g2, [x16[h, ch:] for h in range(r - 1, r + 2)], acts[r - 1])
    g2_out[...] = g2


def outer_body(
    wf, x16, own, xi, xc, hids, g1_in, g2_in,
    strip_a, strip_b, row_a, row_b, corner_a, corner_b,
    acts_o, hids_o, mine, other, xo, grads,
):
    rows, ch2, cols = x16.shape
    ch = ch2 // 2
    has_north, has_south, has_west, has_east = has_neighbours()
    west, east = side_strips(strip_a, strip_b)
    lane2 = lanes_of((ch2, LANES))
    above, below = sides(
        corner_a[...].astype(F32), None if corner_b is None else corner_b[...].astype(F32), "row"
    )
    corner = jnp.where(lane2 % SLOT < 4, above, below)
    west = west + jnp.where(lane2 < SLOT, corner, 0.0)
    east = east + jnp.where(lane2 < SLOT, pltpu.roll(corner, SLOT, 1), 0.0)
    north, south = sides(row_a[...], None if row_b is None else row_b[...], "row")
    left, right = own[0].astype(F32), own[1].astype(F32)
    first = lanes_of((ch, LANES)) == 0
    last = lanes_of((ch, LANES)) == LANES - 1
    near = jnp.where(even_lanes(west.shape), east, west).astype(BF)
    for k in range(4):
        slot = k if k < 2 else rows + k
        row = (north if k < 2 else south)[k % 2]
        lo, hi = row[:, :LANES].astype(F32), row[:, cols - LANES :].astype(F32)
        left = jnp.where(lane2 == 2 * slot, pltpu.roll(lo, 2 * slot, 1), left)
        right = jnp.where(lane2 == 2 * slot + 1, pltpu.roll(hi, (2 * slot + 2) % LANES, 1), right)
        edge = edge_of(near, slot - 2)
        for which in range(2):
            s = slice(which * ch, (which + 1) * ch)
            put_shifted(xo.at[which], k, halves_of(row[s]), edge[s], first, last)
    lane = lanes_of((ch, LANES))
    slots = lane // 2
    keep = jnp.where(lane % 2 == 0, has_west, has_east)
    keep = keep * jnp.where(slots == 1, has_north, 1.0) * jnp.where(slots == rows + 2, has_south, 1.0)
    sides_of = lambda s: (west[s], east[s], left[s], right[s])
    act_e, hid_e = activation(
        border(wf[0, :ch, : 9 * ch], *sides_of(slice(0, ch))),
        border(wf[1, :ch, : 9 * ch], *sides_of(slice(ch, ch2))),
    )
    act_e = crossed(jnp.where(keep > 0.0, act_e, 0.0))
    hid_e = crossed(jnp.where(keep > 0.0, hid_e, 0.0))
    for t in range(2):
        stacks = []
        for which, mid in enumerate((xi, xc)):
            ends = xo[which, 2 * t : 2 * t + 2].reshape(6 * ch, cols)
            if t == 0:
                stack = [ends, mid[0:2].reshape(6 * ch, cols)]
            else:
                stack = [mid[rows - 2 : rows].reshape(6 * ch, cols), ends]
            stacks.append(jnp.concatenate(stack, 0))
        hidden = jnp.dot(wf[0], stacks[0], preferred_element_type=F32)
        act_grad = jnp.dot(wf[1], stacks[1], preferred_element_type=F32)
        for values, dst, e in zip(activation(hidden, act_grad), (acts_o, hids_o), (act_e, hid_e)):
            for p in range(2):
                at = 2 * t + p
                h = at - 1 if t == 0 else rows - 3 + at
                v = values[p * ch : (p + 1) * ch]
                if at == 0:
                    v = jnp.where(has_north > 0.0, v, 0.0)
                if at == 3:
                    v = jnp.where(has_south > 0.0, v, 0.0)
                put_shifted(
                    dst, at, halves_of(v.astype(BF)), edge_of(e, h), first, last
                )
    zero_row = jnp.zeros((ch, cols), BF)
    g1, g2 = g1_in[...], g2_in[...]
    for k, r in ((0, -1), (1, 0), (2, rows - 1), (3, rows)):
        lhs = [x16[h, ch:] if 0 <= h < rows else zero_row for h in range(r - 1, r + 2)]
        g2 = add_grads(g2, lhs, acts_o[k])
    for h, row in ((0, hids_o[1, ch : 2 * ch]), (rows - 1, hids_o[2, ch : 2 * ch])):
        for r in range(h - 1, h + 2):
            rhs = xi[r] if 0 <= r < rows else xo[0, 1 if r < 0 else 2]
            lhs = [row if h == r - 1 + k else zero_row for k in range(3)]
            g1 = add_grads(g1, lhs, rhs)
    grads[0 : 3 * ch, :] = g1[:, : 2 * ch]
    grads[3 * ch : 6 * ch, :] = g2[:, : 2 * ch]
    grads[6 * ch : 9 * ch, :] = jnp.concatenate([g1[:, 2 * ch :], g2[:, 2 * ch :]], 1)
    count = mine.shape[0]
    core = lax.axis_index("dp") % 2
    mine[...] = grads[pl.ds(core * count, count), :]
    other[...] = grads[pl.ds((1 - core) * count, count), :]


def back_body(flip, kernel, mid, ends, out, weights, wide):
    rows = mid.shape[0] + 2
    ch = kernel.shape[2]
    cols = mid.shape[2]
    pitch = wide.shape[1] // (ch + 1)
    row_weights(weights, kernel, flip)
    for t in range(rows // 2):
        if t == 0:
            stack = jnp.concatenate([ends[0:2], mid[0:2]], 0)
        elif t == rows // 2 - 1:
            stack = jnp.concatenate([mid[rows - 4 : rows - 2], ends[2:4]], 0)
        else:
            stack = mid[2 * t - 2 : 2 * t + 2]
        y = jnp.dot(weights[...], stack.reshape(12 * ch, cols), preferred_element_type=F32)
        for p in range(2):
            for half, part in enumerate(halves_of(y[p * ch : (p + 1) * ch])):
                wide[half, pl.ds(2 * t + p, ch, stride=pitch), :] = part
    for half in range(cols // LANES):
        for c in range(ch):
            out[0, c, :, half * LANES : (half + 1) * LANES] = wide[
                half, c * pitch : c * pitch + rows, :
            ].astype(BF)


def finish_body(factor, mine, other, first, second):
    core = lax.axis_index("dp") % 2
    m, o = mine[...].astype(F32) * factor, other[...].astype(F32) * factor
    whole = jnp.concatenate([jnp.where(core == 0, m, o), jnp.where(core == 0, o, m)], 0)
    ch = first.shape[2]
    tail = whole[6 * ch :]
    swapped = pltpu.roll(whole, LANES - ch, 1)
    for k, dst in ((0, first), (1, second)):
        for a in range(3):
            src = (2 - a) * ch
            dst[a, 0] = whole[k * 3 * ch + src : k * 3 * ch + src + ch, :ch]
            dst[a, 1] = swapped[k * 3 * ch + src : k * 3 * ch + src + ch, :ch]
            third = tail if k == 0 else swapped[6 * ch :]
            dst[a, 2] = third[src : src + ch, :ch]


def exchange(half, dims):
    axes = ("dp", "row", "col")
    sizes = [lax.axis_size(a) for a in axes]
    sent = half.astype(BF)
    total = sent.astype(F32)
    for pick in range(1, 1 << len(dims)):
        flips = [0, 0, 0]
        for k, (axis, bit) in enumerate(dims):
            if pick >> k & 1:
                flips[axis] ^= bit
        perm = []
        for d in range(sizes[0]):
            for r in range(sizes[1]):
                for c in range(sizes[2]):
                    to = (d ^ flips[0], r ^ flips[1], c ^ flips[2])
                    perm.append(
                        ((d * sizes[1] + r) * sizes[2] + c, (to[0] * sizes[1] + to[1]) * sizes[2] + to[2])
                    )
        total = total + lax.ppermute(sent, axes, perm).astype(F32)
    return total


def on_device(images, first_kernel, second_kernel, cotangent):
    ch, rows, cols = images.shape[1:]
    n_row, n_col, n_dp = (lax.axis_size(a) for a in ("row", "col", "dp"))
    total = rows * cols * n_row * n_col * n_dp * images.shape[0]
    factor = 1.0 / math.sqrt(total)
    pitch = 24
    halves = cols // LANES
    two_rows = n_row > 2
    two_cols = n_col > 2
    sds = jax.ShapeDtypeStruct
    strip = sds((2 * ch, LANES), BF)
    row_pair = sds((2, 2 * ch, cols), BF)
    hbm = pl.BlockSpec(memory_space=pltpu.HBM)

    def optional(body, flags):
        def wrapped(*refs):
            refs = list(refs)
            return body(*[refs.pop(0) if keep else None for keep in flags], *refs)

        return wrapped

    k1 = first_kernel.transpose(2, 3, 0, 1)
    k2 = second_kernel.transpose(2, 3, 0, 1)
    pack = kernel_call(
        optional(pack_body, [True] * 11 + [two_rows]),
        [sds((rows, 2 * ch, cols), BF), sds((2, 2 * ch, LANES), BF)]
        + [sds(k1.shape, BF), sds(k2.shape, BF), strip, strip]
        + [row_pair] * (1 + two_rows),
        [
            pltpu.VMEM((2, ch, rows, cols), BF),
            pltpu.VMEM((2, halves, (ch + 1) * pitch, LANES), F32),
            pltpu.SemaphoreType.DMA((2, PIECES)),
            pltpu.SemaphoreType.DMA((2,)),
        ],
        in_specs=[hbm] * 4,
        flops=1 << 27,
        name="pack",
    )
    x16, own, taps1, taps2, send_a, send_b, *row_sends = pack(
        *[pltpu.with_memory_space_constraint(v, pltpu.HBM) for v in (images, cotangent, k1, k2)]
    )
    strips = [swap(send_a, "col", False)]
    if two_cols:
        strips.append(swap(send_b, "col", True))
    got_rows = [swap(s, "row", k == 1) for k, s in enumerate(row_sends)]
    corner_sends = kernel_call(
        optional(functools.partial(corner_body, rows), [True, two_cols, True, two_rows]),
        [strip] * (1 + two_rows),
        name="corner",
    )(*strips)
    corners = [swap(s, "row", k == 1) for k, s in enumerate(corner_sends)]
    shifted = lambda n: sds((n, 3 * ch, cols), BF)
    sums = sds((3 * ch, 3 * ch), F32)
    xi, xc, acts, hids, g1, g2, wf = kernel_call(
        optional(inner_body, [True] * 5 + [two_cols]),
        [shifted(rows), shifted(rows), shifted(rows - 2), shifted(rows - 2), sums, sums]
        + [sds((2, 2 * ch, 12 * ch), BF)],
        flops=1 << 30,
        name="inner",
    )(taps1, taps2, x16, own, *strips)
    half = sds((9 * ch // 2, LANES), F32)
    acts_o, hids_o, mine, other = kernel_call(
        optional(outer_body, [True] * 8 + [True, two_cols] + [True, two_rows] * 2),
        [shifted(4), shifted(4), half, half],
        [pltpu.VMEM((2, 4, 3 * ch, cols), BF), pltpu.VMEM((9 * ch, LANES), F32)],
        flops=1 << 28,
        name="outer",
    )(wf, x16, own, xi, xc, hids, g1, g2, *strips, *got_rows, *corners)

    def back(kernel, mid, ends, flip, name):
        return kernel_call(
            functools.partial(back_body, flip),
            [sds(images.shape, BF)],
            [
                pltpu.VMEM((2 * ch, 12 * ch), BF),
                pltpu.VMEM((halves, (ch + 1) * pitch, LANES), F32),
            ],
            flops=1 << 29,
            name=name,
        )(kernel, mid, ends)[0]

    partner = [(i, i ^ 1) for i in range(n_dp)]
    total_half = mine + lax.ppermute(other, "dp", partner)
    steps = [(0, 1 << k) for k in range(1, n_dp.bit_length() - 1)]
    steps += [(1, 1 << k) for k in range(n_row.bit_length() - 1)]
    steps += [(2, 1 << k) for k in range(n_col.bit_length() - 1)]
    out = back(taps2, acts, acts_o, False, "out")
    grad_in = back(taps1, hids, hids_o, True, "grad_in")
    stages = [steps[k : k + 2] for k in range(0, len(steps), 2)]
    for k, stage in enumerate(stages):
        total_half = exchange(total_half, stage)
        if k == len(stages) - 2:
            total_half, out = lax.optimization_barrier((total_half, out))
        if k == len(stages) - 1:
            total_half, grad_in = lax.optimization_barrier((total_half, grad_in))
    rest = lax.ppermute(total_half, "dp", partner)
    taps = sds((3, 3, ch, ch), F32)
    first, second = kernel_call(
        functools.partial(finish_body, factor), [taps, taps], name="finish"
    )(total_half, rest)
    return out, grad_in, first.transpose(2, 3, 0, 1), second.transpose(2, 3, 0, 1)


def solution(mesh):
    in_specs = (P("dp", None, "row", "col"), P(), P(), P("dp", None, "row", "col"))
    out_specs = (P("dp", None, "row", "col"), P("dp", None, "row", "col"), P(), P())
    return jax.shard_map(
        on_device, mesh=mesh, in_specs=in_specs, out_specs=out_specs, check_vma=False
    )
```

```python
import functools
import math

import jax
import jax.numpy as jnp
from jax import lax
from jax.experimental import pallas as pl
from jax.experimental.pallas import tpu as pltpu
from jax.sharding import PartitionSpec as P

BF = jnp.bfloat16
F32 = jnp.float32
LANES = 128
SLOT = LANES // 2
PIECES = 2


def kernel_call(body, outs, scratch=(), flops=0, name=None, **more):
    return pl.pallas_call(
        body,
        out_shape=outs,
        **more,
        scratch_shapes=list(scratch),
        cost_estimate=pl.CostEstimate(flops=flops, transcendentals=0, bytes_accessed=1 << 20),
        compiler_params=pltpu.CompilerParams(vmem_limit_bytes=24 << 20),
        name=name,
    )


def lanes_of(shape):
    return lax.broadcasted_iota(jnp.int32, shape, len(shape) - 1)


def pairs(size, second):
    out = list(range(size))
    for i in range(1 if second else 0, size - 1, 2):
        out[i], out[i + 1] = i + 1, i
    return out


def swap(array, axis, second):
    size, n_dp = lax.axis_size(axis), lax.axis_size("dp")
    partner = pairs(size, second)
    if partner == list(range(size)):
        return None
    lone = lambda d: d ^ 1 if (d | 1) < n_dp else d
    perm = []
    for d in range(n_dp):
        for i, to in enumerate(partner):
            perm.append((d * size + i, (lone(d) if to == i else d) * size + to))
    return lax.ppermute(array, ("dp", axis), perm)


def pack_body(
    img, cot, k1, k2, x16, own, taps1, taps2, send_a, send_b, row_a, row_b,
    staged, wide, sems, tap_sems,
):
    ch, rows, cols = img.shape[1:]
    halves = cols // LANES
    pitch = wide.shape[2] // (ch + 1)
    col_odd = lax.axis_index("col") % 2 == 1
    row_odd = lax.axis_index("row") % 2 == 1
    lane = lanes_of((ch, LANES))
    cut = ch // PIECES
    tap_copies = [
        pltpu.make_async_copy(src, dst, tap_sems.at[k])
        for k, (src, dst) in enumerate(((k1, taps1), (k2, taps2)))
    ]
    for copy in tap_copies:
        copy.start()
    copies = []
    for which, ref in enumerate((img, cot)):
        for k in range(PIECES):
            span = pl.ds(k * cut, cut)
            copy = pltpu.make_async_copy(
                ref.at[0, span], staged.at[which, span], sems.at[which, k]
            )
            copy.start()
            copies.append(copy)
    for which in range(2):
        base = which * ch
        left = jnp.zeros((ch, LANES), F32)
        right = jnp.zeros((ch, LANES), F32)
        for k in range(PIECES):
            copies[which * PIECES + k].wait()
            for c in range(k * cut, (k + 1) * cut):
                for half in range(halves):
                    wide[which, half, c * pitch : c * pitch + rows, :] = staged[
                        which, c, :, half * LANES : (half + 1) * LANES
                    ].astype(F32)
        for half in range(halves):
            for h in range(rows):
                v = wide[which, half, pl.ds(h, ch, stride=pitch), :]
                x16[h, base : base + ch, half * LANES : (half + 1) * LANES] = v.astype(BF)
                at = 2 * (h + 2)
                here = (lane >= at) & (lane < at + 2)
                if half == 0:
                    left = jnp.where(here, pltpu.roll(v, at, 1), left)
                if half == halves - 1:
                    right = jnp.where(here, pltpu.roll(v, (at + 2) % LANES, 1), right)
        own[0, base : base + ch, :] = left.astype(BF)
        own[1, base : base + ch, :] = right.astype(BF)
        send_a[base : base + ch, :] = jnp.where(col_odd, left, right).astype(BF)
        send_b[base : base + ch, :] = jnp.where(col_odd, right, left).astype(BF)
    row_a[...] = x16[pl.ds(jnp.where(row_odd, 0, rows - 2), 2)]
    if row_b is not None:
        row_b[...] = x16[pl.ds(jnp.where(row_odd, rows - 2, 0), 2)]
    for copy in tap_copies:
        copy.wait()


def sides(a, b, axis):
    at, size = lax.axis_index(axis), lax.axis_size(axis)
    b = a if b is None else b
    odd = at % 2 == 1
    zero = jnp.zeros(a.shape, a.dtype)
    before = jnp.where(at > 0, jnp.where(odd, a, b), zero)
    behind = jnp.where(at < size - 1, jnp.where(odd, b, a), zero)
    return before, behind


def corner_body(rows, strip_a, strip_b, send_a, send_b):
    row_odd = lax.axis_index("row") % 2 == 1
    lane = lanes_of(strip_a.shape)
    west, east = side_strips(strip_a, strip_b)
    both = jnp.where(lane < SLOT, west, pltpu.roll(east, SLOT, 1))
    slot = lane % SLOT
    down = jnp.where(slot < 4, pltpu.roll(both, (-2 * rows) % LANES, 1), 0.0)
    far = (slot >= 2 * (rows + 2)) & (slot < 2 * (rows + 4))
    up = jnp.where(far, pltpu.roll(both, (2 * rows) % LANES, 1), 0.0)
    send_a[...] = jnp.where(row_odd, up, down).astype(BF)
    if send_b is not None:
        send_b[...] = jnp.where(row_odd, down, up).astype(BF)


def put_shifted(dst, at, half_values, edge, first, last):
    ch = half_values[0].shape[0]
    n = len(half_values)
    fwd = [pltpu.roll(v, 1, 1) for v in half_values]
    back = [pltpu.roll(v, LANES - 1, 1) for v in half_values]
    for k in range(n):
        at_lanes = slice(k * LANES, (k + 1) * LANES)
        before = edge if k == 0 else fwd[k - 1]
        after = edge if k == n - 1 else back[k + 1]
        dst[at, 0:ch, at_lanes] = jnp.where(first, before, fwd[k]).astype(BF)
        dst[at, ch : 2 * ch, at_lanes] = half_values[k].astype(BF)
        dst[at, 2 * ch : 3 * ch, at_lanes] = jnp.where(last, after, back[k]).astype(BF)


def halves_of(v):
    return [v[:, k * LANES : (k + 1) * LANES] for k in range(v.shape[1] // LANES)]


def has_neighbours():
    out = []
    for axis in ("row", "col"):
        at, size = lax.axis_index(axis), lax.axis_size(axis)
        out += [jnp.where(at > 0, 1.0, 0.0), jnp.where(at < size - 1, 1.0, 0.0)]
    return out


def side_strips(strip_a, strip_b):
    return sides(
        strip_a[...].astype(F32),
        None if strip_b is None else strip_b[...].astype(F32),
        "col",
    )


def even_lanes(shape):
    return lanes_of(shape) % 2 == 0


def edge_of(strips, h):
    return pltpu.roll(strips, (-2 * (h + 2) - 1) % LANES, 1)


def border(weights, west, east, left, right):
    even = even_lanes(west.shape)
    b0 = jnp.where(even, west, right)
    b1 = jnp.where(even, pltpu.roll(west, LANES - 1, 1), pltpu.roll(east, 1, 1))
    b2 = jnp.where(even, left, east)
    taps = []
    for a in range(3):
        taps += [pltpu.roll(b, (2 - 2 * a) % LANES, 1) if a != 1 else b for b in (b0, b1, b2)]
    stack = jnp.concatenate(taps, 0).astype(BF)
    return jnp.dot(weights, stack, preferred_element_type=F32)


def crossed(strips):
    v = strips.astype(BF)
    return jnp.where(even_lanes(v.shape), pltpu.roll(v, LANES - 1, 1), pltpu.roll(v, 1, 1))


def activation(hidden, act_grad):
    s = 0.5 * jnp.tanh(0.5 * hidden) + 0.5
    return hidden * s, act_grad * (s * (1.0 + hidden * (1.0 - s)))


def row_weights(dst, kernel, flip):
    ch = kernel.shape[2]
    zero = jnp.zeros((ch, ch), BF)
    taps = []
    for a in range(3):
        for b in range(3):
            taps.append(kernel[2 - a, 2 - b].T if flip else kernel[a, b])
    for p in range(2):
        blocks = [zero] * (3 * p) + taps + [zero] * (3 - 3 * p)
        for k in range(6):
            dst[p * ch : (p + 1) * ch, k * LANES : (k + 1) * LANES] = jnp.concatenate(
                blocks[2 * k : 2 * k + 2], 1
            )


NT = (((1,), (1,)), ((), ()))


def add_grads(sums, lhs_rows, rhs):
    lhs = jnp.concatenate(lhs_rows, 0)
    return sums + lax.dot_general(lhs, rhs, NT, preferred_element_type=F32)


def inner_body(
    taps1, taps2, x16, own, strip_a, strip_b,
    xi, xc, acts, hids, g1_out, g2_out, wf,
):
    rows, ch2, cols = x16.shape
    ch = ch2 // 2
    row_weights(wf.at[0], taps1, False)
    row_weights(wf.at[1], taps2, True)
    west, east = side_strips(strip_a, strip_b)
    left, right = own[0].astype(F32), own[1].astype(F32)
    first = lanes_of((ch, LANES)) == 0
    last = lanes_of((ch, LANES)) == LANES - 1
    near = jnp.where(even_lanes(west.shape), east, west).astype(BF)
    for h in range(rows):
        edge = edge_of(near, h)
        for which, dst in enumerate((xi, xc)):
            s = slice(which * ch, (which + 1) * ch)
            put_shifted(dst, h, halves_of(x16[h, s]), edge[s], first, last)
    lane = lanes_of((ch, LANES))
    _, _, has_west, has_east = has_neighbours()
    keep = jnp.where(lane % 2 == 0, has_west, has_east) > 0.0
    sides_of = lambda s: (west[s], east[s], left[s], right[s])
    hidden_e = border(wf[0, :ch, : 9 * ch], *sides_of(slice(0, ch)))
    act_e = crossed(jnp.where(keep, activation(hidden_e, hidden_e)[0], 0.0))
    zero_row = jnp.zeros((ch, cols), BF)
    for t in range((rows - 2) // 2):
        at = 2 * t
        hidden = jnp.dot(
            wf[0], xi[at : at + 4].reshape(12 * ch, cols), preferred_element_type=F32
        )
        act_grad = jnp.dot(
            wf[1], xc[at : at + 4].reshape(12 * ch, cols), preferred_element_type=F32
        )
        act, hid = [v.astype(BF) for v in activation(hidden, act_grad)]
        for p in range(2):
            own_rows = slice(p * ch, (p + 1) * ch)
            hids[at + p] = hid[own_rows]
            put_shifted(
                acts, at + p, halves_of(act[own_rows]), edge_of(act_e, at + p + 1), first, last
            )
    g1 = jnp.zeros((3 * ch, 3 * ch), F32)
    for r in range(rows):
        lhs = [
            hids[h - 1] if 1 <= h <= rows - 2 else zero_row for h in range(r - 1, r + 2)
        ]
        g1 = add_grads(g1, lhs, xi[r])
    g1_out[...] = g1
    g2 = jnp.zeros((3 * ch, 3 * ch), F32)
    for r in range(1, rows - 1):
        g2 = add_grads(g2, [x16[h, ch:] for h in range(r - 1, r + 2)], acts[r - 1])
    g2_out[...] = g2


def outer_body(
    wf, x16, own, xi, xc, hids, g1_in, g2_in,
    strip_a, strip_b, row_a, row_b, corner_a, corner_b,
    acts_o, hids_o, hid_edge, mine, other, xo,
):
    rows, ch2, cols = x16.shape
    ch = ch2 // 2
    has_north, has_south, has_west, has_east = has_neighbours()
    west, east = side_strips(strip_a, strip_b)
    lane2 = lanes_of((ch2, LANES))
    above, below = sides(
        corner_a[...].astype(F32), None if corner_b is None else corner_b[...].astype(F32), "row"
    )
    corner = jnp.where(lane2 % SLOT < 4, above, below)
    west = west + jnp.where(lane2 < SLOT, corner, 0.0)
    east = east + jnp.where(lane2 < SLOT, pltpu.roll(corner, SLOT, 1), 0.0)
    north, south = sides(row_a[...], None if row_b is None else row_b[...], "row")
    left, right = own[0].astype(F32), own[1].astype(F32)
    first = lanes_of((ch, LANES)) == 0
    last = lanes_of((ch, LANES)) == LANES - 1
    near = jnp.where(even_lanes(west.shape), east, west).astype(BF)
    for k in range(4):
        slot = k if k < 2 else rows + k
        row = (north if k < 2 else south)[k % 2]
        lo, hi = row[:, :LANES].astype(F32), row[:, cols - LANES :].astype(F32)
        left = jnp.where(lane2 == 2 * slot, pltpu.roll(lo, 2 * slot, 1), left)
        right = jnp.where(lane2 == 2 * slot + 1, pltpu.roll(hi, (2 * slot + 2) % LANES, 1), right)
        edge = edge_of(near, slot - 2)
        for which in range(2):
            s = slice(which * ch, (which + 1) * ch)
            put_shifted(xo.at[which], k, halves_of(row[s]), edge[s], first, last)
    lane = lanes_of((ch, LANES))
    slots = lane // 2
    keep = jnp.where(lane % 2 == 0, has_west, has_east)
    keep = keep * jnp.where(slots == 1, has_north, 1.0) * jnp.where(slots == rows + 2, has_south, 1.0)
    sides_of = lambda s: (west[s], east[s], left[s], right[s])
    act_e, hid_e = activation(
        border(wf[0, :ch, : 9 * ch], *sides_of(slice(0, ch))),
        border(wf[1, :ch, : 9 * ch], *sides_of(slice(ch, ch2))),
    )
    act_e = crossed(jnp.where(keep > 0.0, act_e, 0.0))
    hid_edge[...] = crossed(jnp.where(keep > 0.0, hid_e, 0.0))
    for t in range(2):
        stacks = []
        for which, mid in enumerate((xi, xc)):
            ends = xo[which, 2 * t : 2 * t + 2].reshape(6 * ch, cols)
            if t == 0:
                stack = [ends, mid[0:2].reshape(6 * ch, cols)]
            else:
                stack = [mid[rows - 2 : rows].reshape(6 * ch, cols), ends]
            stacks.append(jnp.concatenate(stack, 0))
        hidden = jnp.dot(wf[0], stacks[0], preferred_element_type=F32)
        act_grad = jnp.dot(wf[1], stacks[1], preferred_element_type=F32)
        for values, dst in zip(activation(hidden, act_grad), (acts_o, hids_o)):
            for p in range(2):
                at = 2 * t + p
                h = at - 1 if t == 0 else rows - 3 + at
                v = values[p * ch : (p + 1) * ch]
                if at == 0:
                    v = jnp.where(has_north > 0.0, v, 0.0)
                if at == 3:
                    v = jnp.where(has_south > 0.0, v, 0.0)
                if dst is hids_o:
                    dst[at] = v.astype(BF)
                else:
                    put_shifted(dst, at, halves_of(v.astype(BF)), edge_of(act_e, h), first, last)
    zero_row = jnp.zeros((ch, cols), BF)
    g1, g2 = g1_in[...], g2_in[...]
    for k, r in ((0, -1), (1, 0), (2, rows - 1), (3, rows)):
        lhs = [x16[h, ch:] if 0 <= h < rows else zero_row for h in range(r - 1, r + 2)]
        g2 = add_grads(g2, lhs, acts_o[k])
    for h, row in ((0, hids_o[1]), (rows - 1, hids_o[2])):
        for r in range(h - 1, h + 2):
            rhs = xi[r] if 0 <= r < rows else xo[0, 1 if r < 0 else 2]
            lhs = [row if h == r - 1 + k else zero_row for k in range(3)]
            g1 = add_grads(g1, lhs, rhs)
    count = mine.shape[0]
    cut = count - 3 * ch
    low = jnp.concatenate([g1[:, : 2 * ch], g2[:cut, : 2 * ch]], 0)
    tail = jnp.concatenate([g1[:, 2 * ch :], g2[:, 2 * ch :]], 1)
    high = jnp.concatenate([g2[cut:, : 2 * ch], tail], 0)
    leads = lax.axis_index("dp") % 2 == 0
    mine[...] = jnp.where(leads, low, high)
    other[...] = jnp.where(leads, high, low)


def back_body(flip, kernel, mid, ends, edge, out, weights, wide, shifted):
    rows = mid.shape[0] + 2
    ch = kernel.shape[2]
    cols = mid.shape[2]
    pitch = wide.shape[1] // (ch + 1)
    row_weights(weights, kernel, flip)
    if edge is not None:
        first = lanes_of((ch, LANES)) == 0
        last = lanes_of((ch, LANES)) == LANES - 1
        for at in range(rows + 2):
            row = ends[at] if at < 2 else mid[at - 2] if at < rows else ends[at - rows + 2]
            put_shifted(shifted, at, halves_of(row), edge_of(edge[...], at - 1), first, last)
    for t in range(rows // 2):
        if edge is not None:
            stack = shifted[2 * t : 2 * t + 4]
        elif t == 0:
            stack = jnp.concatenate([ends[0:2], mid[0:2]], 0)
        elif t == rows // 2 - 1:
            stack = jnp.concatenate([mid[rows - 4 : rows - 2], ends[2:4]], 0)
        else:
            stack = mid[2 * t - 2 : 2 * t + 2]
        y = jnp.dot(weights[...], stack.reshape(12 * ch, cols), preferred_element_type=F32)
        for p in range(2):
            for half, part in enumerate(halves_of(y[p * ch : (p + 1) * ch])):
                wide[half, pl.ds(2 * t + p, ch, stride=pitch), :] = part
    for half in range(cols // LANES):
        for c in range(ch):
            out[0, c, :, half * LANES : (half + 1) * LANES] = wide[
                half, c * pitch : c * pitch + rows, :
            ].astype(BF)


def finish_body(factor, mine, other, first, second):
    core = lax.axis_index("dp") % 2
    m, o = mine[...].astype(F32) * factor, other[...].astype(F32) * factor
    whole = jnp.concatenate([jnp.where(core == 0, m, o), jnp.where(core == 0, o, m)], 0)
    ch = first.shape[2]
    tail = whole[6 * ch :]
    swapped = pltpu.roll(whole, LANES - ch, 1)
    for k, dst in ((0, first), (1, second)):
        for a in range(3):
            src = (2 - a) * ch
            dst[a, 0] = whole[k * 3 * ch + src : k * 3 * ch + src + ch, :ch]
            dst[a, 1] = swapped[k * 3 * ch + src : k * 3 * ch + src + ch, :ch]
            third = tail if k == 0 else swapped[6 * ch :]
            dst[a, 2] = third[src : src + ch, :ch]


def exchange(half, dims):
    axes = ("dp", "row", "col")
    sizes = [lax.axis_size(a) for a in axes]
    sent = half.astype(BF)
    total = sent.astype(F32)
    for pick in range(1, 1 << len(dims)):
        flips = [0, 0, 0]
        for k, (axis, bit) in enumerate(dims):
            if pick >> k & 1:
                flips[axis] ^= bit
        perm = []
        for d in range(sizes[0]):
            for r in range(sizes[1]):
                for c in range(sizes[2]):
                    to = (d ^ flips[0], r ^ flips[1], c ^ flips[2])
                    perm.append(
                        ((d * sizes[1] + r) * sizes[2] + c, (to[0] * sizes[1] + to[1]) * sizes[2] + to[2])
                    )
        total = total + lax.ppermute(sent, axes, perm).astype(F32)
    return total


def on_device(images, first_kernel, second_kernel, cotangent):
    ch, rows, cols = images.shape[1:]
    n_row, n_col, n_dp = (lax.axis_size(a) for a in ("row", "col", "dp"))
    total = rows * cols * n_row * n_col * n_dp * images.shape[0]
    factor = 1.0 / math.sqrt(total)
    pitch = 24
    halves = cols // LANES
    two_rows = n_row > 2
    two_cols = n_col > 2
    sds = jax.ShapeDtypeStruct
    strip = sds((2 * ch, LANES), BF)
    row_pair = sds((2, 2 * ch, cols), BF)
    hbm = pl.BlockSpec(memory_space=pltpu.HBM)

    def optional(body, flags):
        def wrapped(*refs):
            refs = list(refs)
            return body(*[refs.pop(0) if keep else None for keep in flags], *refs)

        return wrapped

    k1 = first_kernel.transpose(2, 3, 0, 1)
    k2 = second_kernel.transpose(2, 3, 0, 1)
    pack = kernel_call(
        optional(pack_body, [True] * 11 + [two_rows]),
        [sds((rows, 2 * ch, cols), BF), sds((2, 2 * ch, LANES), BF)]
        + [sds(k1.shape, BF), sds(k2.shape, BF), strip, strip]
        + [row_pair] * (1 + two_rows),
        [
            pltpu.VMEM((2, ch, rows, cols), BF),
            pltpu.VMEM((2, halves, (ch + 1) * pitch, LANES), F32),
            pltpu.SemaphoreType.DMA((2, PIECES)),
            pltpu.SemaphoreType.DMA((2,)),
        ],
        in_specs=[hbm] * 4,
        flops=1 << 27,
        name="pack",
    )
    x16, own, taps1, taps2, send_a, send_b, *row_sends = pack(
        *[pltpu.with_memory_space_constraint(v, pltpu.HBM) for v in (images, cotangent, k1, k2)]
    )
    strips = [swap(send_a, "col", False)]
    if two_cols:
        strips.append(swap(send_b, "col", True))
    got_rows = [swap(s, "row", k == 1) for k, s in enumerate(row_sends)]
    corner_sends = kernel_call(
        optional(functools.partial(corner_body, rows), [True, two_cols, True, two_rows]),
        [strip] * (1 + two_rows),
        name="corner",
    )(*strips)
    corners = [swap(s, "row", k == 1) for k, s in enumerate(corner_sends)]
    shifted = lambda n: sds((n, 3 * ch, cols), BF)
    sums = sds((3 * ch, 3 * ch), F32)
    xi, xc, acts, hids, g1, g2, wf = kernel_call(
        optional(inner_body, [True] * 5 + [two_cols]),
        [shifted(rows), shifted(rows), shifted(rows - 2), sds((rows - 2, ch, cols), BF), sums, sums]
        + [sds((2, 2 * ch, 12 * ch), BF)],
        flops=1 << 30,
        name="inner",
    )(taps1, taps2, x16, own, *strips)
    half = sds((9 * ch // 2, LANES), F32)
    acts_o, hids_o, hid_edge, mine, other = kernel_call(
        optional(outer_body, [True] * 8 + [True, two_cols] + [True, two_rows] * 2),
        [shifted(4), sds((4, ch, cols), BF), sds((ch, LANES), BF), half, half],
        [pltpu.VMEM((2, 4, 3 * ch, cols), BF)],
        flops=1 << 28,
        name="outer",
    )(wf, x16, own, xi, xc, hids, g1, g2, *strips, *got_rows, *corners)

    def back(kernel, mid, ends, flip, name, edge=()):
        scratch = [
            pltpu.VMEM((2 * ch, 12 * ch), BF),
            pltpu.VMEM((halves, (ch + 1) * pitch, LANES), F32),
            pltpu.VMEM((rows + 2, 3 * ch, cols), BF),
        ]
        body = optional(functools.partial(back_body, flip), [True] * 3 + [bool(edge)])
        return kernel_call(body, [sds(images.shape, BF)], scratch, flops=1 << 29, name=name)(
            kernel, mid, ends, *edge
        )[0]

    partner = [(i, i ^ 1) for i in range(n_dp)]
    total_half = mine + lax.ppermute(other, "dp", partner)
    steps = [(0, 1 << k) for k in range(1, n_dp.bit_length() - 1)]
    steps += [(1, 1 << k) for k in range(n_row.bit_length() - 1)]
    steps += [(2, 1 << k) for k in range(n_col.bit_length() - 1)]
    out = back(taps2, acts, acts_o, False, "out")
    grad_in = back(taps1, hids, hids_o, True, "grad_in", (hid_edge,))
    stages = [steps[k : k + 2] for k in range(0, len(steps), 2)]
    for k, stage in enumerate(stages):
        total_half = exchange(total_half, stage)
        if k == len(stages) - 2:
            total_half, out = lax.optimization_barrier((total_half, out))
        if k == len(stages) - 1:
            total_half, grad_in = lax.optimization_barrier((total_half, grad_in))
    rest = lax.ppermute(total_half, "dp", partner)
    taps = sds((3, 3, ch, ch), F32)
    first, second = kernel_call(
        functools.partial(finish_body, factor), [taps, taps], name="finish"
    )(total_half, rest)
    return out, grad_in, first.transpose(2, 3, 0, 1), second.transpose(2, 3, 0, 1)


def solution(mesh):
    in_specs = (P("dp", None, "row", "col"), P(), P(), P("dp", None, "row", "col"))
    out_specs = (P("dp", None, "row", "col"), P("dp", None, "row", "col"), P(), P())
    return jax.shard_map(
        on_device, mesh=mesh, in_specs=in_specs, out_specs=out_specs, check_vma=False
    )
```

```python
import functools
import math

import jax
import jax.numpy as jnp
from jax import lax
from jax.experimental import pallas as pl
from jax.experimental.pallas import tpu as pltpu
from jax.sharding import PartitionSpec as P

BF = jnp.bfloat16
F32 = jnp.float32
LANES = 128
SLOT = LANES // 2
PIECES = 2


def kernel_call(body, outs, scratch=(), flops=0, name=None, **more):
    return pl.pallas_call(
        body,
        out_shape=outs,
        **more,
        scratch_shapes=list(scratch),
        cost_estimate=pl.CostEstimate(flops=flops, transcendentals=0, bytes_accessed=1 << 20),
        compiler_params=pltpu.CompilerParams(vmem_limit_bytes=24 << 20),
        name=name,
    )


def lanes_of(shape):
    return lax.broadcasted_iota(jnp.int32, shape, len(shape) - 1)


def pairs(size, second):
    out = list(range(size))
    for i in range(1 if second else 0, size - 1, 2):
        out[i], out[i + 1] = i + 1, i
    return out


def swap(array, axis, second):
    size, n_dp = lax.axis_size(axis), lax.axis_size("dp")
    partner = pairs(size, second)
    if partner == list(range(size)):
        return None
    lone = lambda d: d ^ 1 if (d | 1) < n_dp else d
    perm = []
    for d in range(n_dp):
        for i, to in enumerate(partner):
            perm.append((d * size + i, (lone(d) if to == i else d) * size + to))
    return lax.ppermute(array, ("dp", axis), perm)


def pack_body(
    img, cot, k1, k2, x16, own, taps1, taps2, send_a, send_b, row_a, row_b,
    staged, wide, sems, tap_sems,
):
    ch, rows, cols = img.shape[1:]
    halves = cols // LANES
    pitch = wide.shape[2] // (ch + 1)
    col_odd = lax.axis_index("col") % 2 == 1
    row_odd = lax.axis_index("row") % 2 == 1
    lane = lanes_of((ch, LANES))
    cut = ch // PIECES
    tap_copies = [
        pltpu.make_async_copy(src, dst, tap_sems.at[k])
        for k, (src, dst) in enumerate(((k1, taps1), (k2, taps2)))
    ]
    for copy in tap_copies:
        copy.start()
    copies = []
    for which, ref in enumerate((img, cot)):
        for k in range(PIECES):
            span = pl.ds(k * cut, cut)
            copy = pltpu.make_async_copy(
                ref.at[0, span], staged.at[which, span], sems.at[which, k]
            )
            copy.start()
            copies.append(copy)
    for which in range(2):
        base = which * ch
        left = jnp.zeros((ch, LANES), F32)
        right = jnp.zeros((ch, LANES), F32)
        for k in range(PIECES):
            copies[which * PIECES + k].wait()
            for c in range(k * cut, (k + 1) * cut):
                for half in range(halves):
                    wide[which, half, c * pitch : c * pitch + rows, :] = staged[
                        which, c, :, half * LANES : (half + 1) * LANES
                    ].astype(F32)
        for half in range(halves):
            for h in range(rows):
                v = wide[which, half, pl.ds(h, ch, stride=pitch), :]
                x16[h, base : base + ch, half * LANES : (half + 1) * LANES] = v.astype(BF)
                at = 2 * (h + 2)
                here = (lane >= at) & (lane < at + 2)
                if half == 0:
                    left = jnp.where(here, pltpu.roll(v, at, 1), left)
                if half == halves - 1:
                    right = jnp.where(here, pltpu.roll(v, (at + 2) % LANES, 1), right)
        own[0, base : base + ch, :] = left.astype(BF)
        own[1, base : base + ch, :] = right.astype(BF)
        send_a[base : base + ch, :] = jnp.where(col_odd, left, right).astype(BF)
        send_b[base : base + ch, :] = jnp.where(col_odd, right, left).astype(BF)
    row_a[...] = x16[pl.ds(jnp.where(row_odd, 0, rows - 2), 2)]
    if row_b is not None:
        row_b[...] = x16[pl.ds(jnp.where(row_odd, rows - 2, 0), 2)]
    for copy in tap_copies:
        copy.wait()


def sides(a, b, axis):
    at, size = lax.axis_index(axis), lax.axis_size(axis)
    b = a if b is None else b
    odd = at % 2 == 1
    zero = jnp.zeros(a.shape, a.dtype)
    before = jnp.where(at > 0, jnp.where(odd, a, b), zero)
    behind = jnp.where(at < size - 1, jnp.where(odd, b, a), zero)
    return before, behind


def corner_body(rows, strip_a, strip_b, send_a, send_b):
    row_odd = lax.axis_index("row") % 2 == 1
    lane = lanes_of(strip_a.shape)
    west, east = side_strips(strip_a, strip_b)
    both = jnp.where(lane < SLOT, west, pltpu.roll(east, SLOT, 1))
    slot = lane % SLOT
    down = jnp.where(slot < 4, pltpu.roll(both, (-2 * rows) % LANES, 1), 0.0)
    far = (slot >= 2 * (rows + 2)) & (slot < 2 * (rows + 4))
    up = jnp.where(far, pltpu.roll(both, (2 * rows) % LANES, 1), 0.0)
    send_a[...] = jnp.where(row_odd, up, down).astype(BF)
    if send_b is not None:
        send_b[...] = jnp.where(row_odd, down, up).astype(BF)


def put_shifted(dst, at, half_values, edge, first, last):
    ch = half_values[0].shape[0]
    n = len(half_values)
    fwd = [pltpu.roll(v, 1, 1) for v in half_values]
    back = [pltpu.roll(v, LANES - 1, 1) for v in half_values]
    for k in range(n):
        at_lanes = slice(k * LANES, (k + 1) * LANES)
        before = edge if k == 0 else fwd[k - 1]
        after = edge if k == n - 1 else back[k + 1]
        dst[at, 0:ch, at_lanes] = jnp.where(first, before, fwd[k]).astype(BF)
        dst[at, ch : 2 * ch, at_lanes] = half_values[k].astype(BF)
        dst[at, 2 * ch : 3 * ch, at_lanes] = jnp.where(last, after, back[k]).astype(BF)


def halves_of(v):
    return [v[:, k * LANES : (k + 1) * LANES] for k in range(v.shape[1] // LANES)]


def has_neighbours():
    out = []
    for axis in ("row", "col"):
        at, size = lax.axis_index(axis), lax.axis_size(axis)
        out += [jnp.where(at > 0, 1.0, 0.0), jnp.where(at < size - 1, 1.0, 0.0)]
    return out


def side_strips(strip_a, strip_b):
    return sides(
        strip_a[...].astype(F32),
        None if strip_b is None else strip_b[...].astype(F32),
        "col",
    )


def even_lanes(shape):
    return lanes_of(shape) % 2 == 0


def edge_of(strips, h):
    return pltpu.roll(strips, (-2 * (h + 2) - 1) % LANES, 1)


def border(weights, west, east, left, right):
    even = even_lanes(west.shape)
    b0 = jnp.where(even, west, right)
    b1 = jnp.where(even, pltpu.roll(west, LANES - 1, 1), pltpu.roll(east, 1, 1))
    b2 = jnp.where(even, left, east)
    taps = []
    for a in range(3):
        taps += [pltpu.roll(b, (2 - 2 * a) % LANES, 1) if a != 1 else b for b in (b0, b1, b2)]
    stack = jnp.concatenate(taps, 0).astype(BF)
    return jnp.dot(weights, stack, preferred_element_type=F32)


def crossed(strips):
    v = strips.astype(BF)
    return jnp.where(even_lanes(v.shape), pltpu.roll(v, LANES - 1, 1), pltpu.roll(v, 1, 1))


def activation(hidden, act_grad):
    s = 0.5 * jnp.tanh(0.5 * hidden) + 0.5
    return hidden * s, act_grad * (s * (1.0 + hidden * (1.0 - s)))


def row_weights(dst, kernel, flip):
    ch = kernel.shape[2]
    zero = jnp.zeros((ch, ch), BF)
    taps = []
    for a in range(3):
        for b in range(3):
            taps.append(kernel[2 - a, 2 - b].T if flip else kernel[a, b])
    for p in range(2):
        blocks = [zero] * (3 * p) + taps + [zero] * (3 - 3 * p)
        for k in range(6):
            dst[p * ch : (p + 1) * ch, k * LANES : (k + 1) * LANES] = jnp.concatenate(
                blocks[2 * k : 2 * k + 2], 1
            )


NT = (((1,), (1,)), ((), ()))


def add_grads(sums, lhs_rows, rhs):
    lhs = jnp.concatenate(lhs_rows, 0)
    return sums + lax.dot_general(lhs, rhs, NT, preferred_element_type=F32)


def inner_body(
    taps1, taps2, x16, own, strip_a, strip_b,
    xi, xc, acts, hids, g1_out, g2_out, wf,
):
    rows, ch2, cols = x16.shape
    ch = ch2 // 2
    row_weights(wf.at[0], taps1, False)
    row_weights(wf.at[1], taps2, True)
    west, east = side_strips(strip_a, strip_b)
    left, right = own[0].astype(F32), own[1].astype(F32)
    first = lanes_of((ch, LANES)) == 0
    last = lanes_of((ch, LANES)) == LANES - 1
    near = jnp.where(even_lanes(west.shape), east, west).astype(BF)
    for h in range(rows):
        edge = edge_of(near, h)
        for which, dst in enumerate((xi, xc)):
            s = slice(which * ch, (which + 1) * ch)
            put_shifted(dst, h, halves_of(x16[h, s]), edge[s], first, last)
    lane = lanes_of((ch, LANES))
    _, _, has_west, has_east = has_neighbours()
    keep = jnp.where(lane % 2 == 0, has_west, has_east) > 0.0
    sides_of = lambda s: (west[s], east[s], left[s], right[s])
    act_e, hid_e = activation(
        border(wf[0, :ch, : 9 * ch], *sides_of(slice(0, ch))),
        border(wf[1, :ch, : 9 * ch], *sides_of(slice(ch, ch2))),
    )
    act_e = crossed(jnp.where(keep, act_e, 0.0))
    hid_e = crossed(jnp.where(keep, hid_e, 0.0))
    zero_row = jnp.zeros((ch, cols), BF)
    for t in range((rows - 2) // 2):
        at = 2 * t
        hidden = jnp.dot(
            wf[0], xi[at : at + 4].reshape(12 * ch, cols), preferred_element_type=F32
        )
        act_grad = jnp.dot(
            wf[1], xc[at : at + 4].reshape(12 * ch, cols), preferred_element_type=F32
        )
        for values, dst, e in zip(activation(hidden, act_grad), (acts, hids), (act_e, hid_e)):
            for p in range(2):
                h = at + p + 1
                put_shifted(
                    dst, at + p, halves_of(values[p * ch : (p + 1) * ch].astype(BF)),
                    edge_of(e, h), first, last,
                )
    g1 = jnp.zeros((3 * ch, 3 * ch), F32)
    for r in range(rows):
        lhs = [
            hids[h - 1, ch : 2 * ch] if 1 <= h <= rows - 2 else zero_row for h in range(r - 1, r + 2)
        ]
        g1 = add_grads(g1, lhs, xi[r])
    g1_out[...] = g1
    g2 = jnp.zeros((3 * ch, 3 * ch), F32)
    for r in range(1, rows - 1):
        g2 = add_grads(g2, [x16[h, ch:] for h in range(r - 1, r + 2)], acts[r - 1])
    g2_out[...] = g2


def outer_body(
    wf, x16, own, xi, xc, hids, g1_in, g2_in,
    strip_a, strip_b, row_a, row_b, corner_a, corner_b,
    acts_o, hids_o, mine, other, xo,
):
    rows, ch2, cols = x16.shape
    ch = ch2 // 2
    has_north, has_south, has_west, has_east = has_neighbours()
    west, east = side_strips(strip_a, strip_b)
    lane2 = lanes_of((ch2, LANES))
    above, below = sides(
        corner_a[...].astype(F32), None if corner_b is None else corner_b[...].astype(F32), "row"
    )
    corner = jnp.where(lane2 % SLOT < 4, above, below)
    west = west + jnp.where(lane2 < SLOT, corner, 0.0)
    east = east + jnp.where(lane2 < SLOT, pltpu.roll(corner, SLOT, 1), 0.0)
    north, south = sides(row_a[...], None if row_b is None else row_b[...], "row")
    left, right = own[0].astype(F32), own[1].astype(F32)
    first = lanes_of((ch, LANES)) == 0
    last = lanes_of((ch, LANES)) == LANES - 1
    near = jnp.where(even_lanes(west.shape), east, west).astype(BF)
    for k in range(4):
        slot = k if k < 2 else rows + k
        row = (north if k < 2 else south)[k % 2]
        lo, hi = row[:, :LANES].astype(F32), row[:, cols - LANES :].astype(F32)
        left = jnp.where(lane2 == 2 * slot, pltpu.roll(lo, 2 * slot, 1), left)
        right = jnp.where(lane2 == 2 * slot + 1, pltpu.roll(hi, (2 * slot + 2) % LANES, 1), right)
        edge = edge_of(near, slot - 2)
        for which in range(2):
            s = slice(which * ch, (which + 1) * ch)
            put_shifted(xo.at[which], k, halves_of(row[s]), edge[s], first, last)
    lane = lanes_of((ch, LANES))
    slots = lane // 2
    keep = jnp.where(lane % 2 == 0, has_west, has_east)
    keep = keep * jnp.where(slots == 1, has_north, 1.0) * jnp.where(slots == rows + 2, has_south, 1.0)
    sides_of = lambda s: (west[s], east[s], left[s], right[s])
    act_e, hid_e = activation(
        border(wf[0, :ch, : 9 * ch], *sides_of(slice(0, ch))),
        border(wf[1, :ch, : 9 * ch], *sides_of(slice(ch, ch2))),
    )
    act_e = crossed(jnp.where(keep > 0.0, act_e, 0.0))
    hid_e = crossed(jnp.where(keep > 0.0, hid_e, 0.0))
    for t in range(2):
        stacks = []
        for which, mid in enumerate((xi, xc)):
            ends = xo[which, 2 * t : 2 * t + 2].reshape(6 * ch, cols)
            if t == 0:
                stack = [ends, mid[0:2].reshape(6 * ch, cols)]
            else:
                stack = [mid[rows - 2 : rows].reshape(6 * ch, cols), ends]
            stacks.append(jnp.concatenate(stack, 0))
        hidden = jnp.dot(wf[0], stacks[0], preferred_element_type=F32)
        act_grad = jnp.dot(wf[1], stacks[1], preferred_element_type=F32)
        for values, dst, e in zip(activation(hidden, act_grad), (acts_o, hids_o), (act_e, hid_e)):
            for p in range(2):
                at = 2 * t + p
                h = at - 1 if t == 0 else rows - 3 + at
                v = values[p * ch : (p + 1) * ch]
                if at == 0:
                    v = jnp.where(has_north > 0.0, v, 0.0)
                if at == 3:
                    v = jnp.where(has_south > 0.0, v, 0.0)
                put_shifted(
                    dst, at, halves_of(v.astype(BF)), edge_of(e, h), first, last
                )
    zero_row = jnp.zeros((ch, cols), BF)
    g1, g2 = g1_in[...], g2_in[...]
    for k, r in ((0, -1), (1, 0), (2, rows - 1), (3, rows)):
        lhs = [x16[h, ch:] if 0 <= h < rows else zero_row for h in range(r - 1, r + 2)]
        g2 = add_grads(g2, lhs, acts_o[k])
    for h, row in ((0, hids_o[1, ch : 2 * ch]), (rows - 1, hids_o[2, ch : 2 * ch])):
        for r in range(h - 1, h + 2):
            rhs = xi[r] if 0 <= r < rows else xo[0, 1 if r < 0 else 2]
            lhs = [row if h == r - 1 + k else zero_row for k in range(3)]
            g1 = add_grads(g1, lhs, rhs)
    count = mine.shape[0]
    cut = count - 3 * ch
    low = jnp.concatenate([g1[:, : 2 * ch], g2[:cut, : 2 * ch]], 0)
    tail = jnp.concatenate([g1[:, 2 * ch :], g2[:, 2 * ch :]], 1)
    high = jnp.concatenate([g2[cut:, : 2 * ch], tail], 0)
    leads = lax.axis_index("dp") % 2 == 0
    mine[...] = jnp.where(leads, low, high)
    other[...] = jnp.where(leads, high, low)


def back_body(flip, kernel, mid, ends, out, weights, wide):
    rows = mid.shape[0] + 2
    ch = kernel.shape[2]
    cols = mid.shape[2]
    pitch = wide.shape[1] // (ch + 1)
    row_weights(weights, kernel, flip)
    for t in range(rows // 2):
        if t == 0:
            stack = jnp.concatenate([ends[0:2], mid[0:2]], 0)
        elif t == rows // 2 - 1:
            stack = jnp.concatenate([mid[rows - 4 : rows - 2], ends[2:4]], 0)
        else:
            stack = mid[2 * t - 2 : 2 * t + 2]
        y = jnp.dot(weights[...], stack.reshape(12 * ch, cols), preferred_element_type=F32)
        for p in range(2):
            for half, part in enumerate(halves_of(y[p * ch : (p + 1) * ch])):
                wide[half, pl.ds(2 * t + p, ch, stride=pitch), :] = part
    for half in range(cols // LANES):
        for c in range(ch):
            out[0, c, :, half * LANES : (half + 1) * LANES] = wide[
                half, c * pitch : c * pitch + rows, :
            ].astype(BF)


def finish_body(factor, mine, other, first, second):
    core = lax.axis_index("dp") % 2
    m, o = mine[...].astype(F32) * factor, other[...].astype(F32) * factor
    whole = jnp.concatenate([jnp.where(core == 0, m, o), jnp.where(core == 0, o, m)], 0)
    ch = first.shape[2]
    tail = whole[6 * ch :]
    swapped = pltpu.roll(whole, LANES - ch, 1)
    for k, dst in ((0, first), (1, second)):
        for a in range(3):
            src = (2 - a) * ch
            dst[a, 0] = whole[k * 3 * ch + src : k * 3 * ch + src + ch, :ch]
            dst[a, 1] = swapped[k * 3 * ch + src : k * 3 * ch + src + ch, :ch]
            third = tail if k == 0 else swapped[6 * ch :]
            dst[a, 2] = third[src : src + ch, :ch]


def exchange(half, dims):
    axes = ("dp", "row", "col")
    sizes = [lax.axis_size(a) for a in axes]
    sent = half.astype(BF)
    total = sent.astype(F32)
    for pick in range(1, 1 << len(dims)):
        flips = [0, 0, 0]
        for k, (axis, bit) in enumerate(dims):
            if pick >> k & 1:
                flips[axis] ^= bit
        perm = []
        for d in range(sizes[0]):
            for r in range(sizes[1]):
                for c in range(sizes[2]):
                    to = (d ^ flips[0], r ^ flips[1], c ^ flips[2])
                    perm.append(
                        ((d * sizes[1] + r) * sizes[2] + c, (to[0] * sizes[1] + to[1]) * sizes[2] + to[2])
                    )
        total = total + lax.ppermute(sent, axes, perm).astype(F32)
    return total


def on_device(images, first_kernel, second_kernel, cotangent):
    ch, rows, cols = images.shape[1:]
    n_row, n_col, n_dp = (lax.axis_size(a) for a in ("row", "col", "dp"))
    total = rows * cols * n_row * n_col * n_dp * images.shape[0]
    factor = 1.0 / math.sqrt(total)
    pitch = 24
    halves = cols // LANES
    two_rows = n_row > 2
    two_cols = n_col > 2
    sds = jax.ShapeDtypeStruct
    strip = sds((2 * ch, LANES), BF)
    row_pair = sds((2, 2 * ch, cols), BF)
    hbm = pl.BlockSpec(memory_space=pltpu.HBM)

    def optional(body, flags):
        def wrapped(*refs):
            refs = list(refs)
            return body(*[refs.pop(0) if keep else None for keep in flags], *refs)

        return wrapped

    k1 = first_kernel.transpose(2, 3, 0, 1)
    k2 = second_kernel.transpose(2, 3, 0, 1)
    pack = kernel_call(
        optional(pack_body, [True] * 11 + [two_rows]),
        [sds((rows, 2 * ch, cols), BF), sds((2, 2 * ch, LANES), BF)]
        + [sds(k1.shape, BF), sds(k2.shape, BF), strip, strip]
        + [row_pair] * (1 + two_rows),
        [
            pltpu.VMEM((2, ch, rows, cols), BF),
            pltpu.VMEM((2, halves, (ch + 1) * pitch, LANES), F32),
            pltpu.SemaphoreType.DMA((2, PIECES)),
            pltpu.SemaphoreType.DMA((2,)),
        ],
        in_specs=[hbm] * 4,
        flops=1 << 27,
        name="pack",
    )
    x16, own, taps1, taps2, send_a, send_b, *row_sends = pack(
        *[pltpu.with_memory_space_constraint(v, pltpu.HBM) for v in (images, cotangent, k1, k2)]
    )
    strips = [swap(send_a, "col", False)]
    if two_cols:
        strips.append(swap(send_b, "col", True))
    got_rows = [swap(s, "row", k == 1) for k, s in enumerate(row_sends)]
    corner_sends = kernel_call(
        optional(functools.partial(corner_body, rows), [True, two_cols, True, two_rows]),
        [strip] * (1 + two_rows),
        name="corner",
    )(*strips)
    corners = [swap(s, "row", k == 1) for k, s in enumerate(corner_sends)]
    shifted = lambda n: sds((n, 3 * ch, cols), BF)
    sums = sds((3 * ch, 3 * ch), F32)
    xi, xc, acts, hids, g1, g2, wf = kernel_call(
        optional(inner_body, [True] * 5 + [two_cols]),
        [shifted(rows), shifted(rows), shifted(rows - 2), shifted(rows - 2), sums, sums]
        + [sds((2, 2 * ch, 12 * ch), BF)],
        flops=1 << 30,
        name="inner",
    )(taps1, taps2, x16, own, *strips)
    half = sds((9 * ch // 2, LANES), F32)
    acts_o, hids_o, mine, other = kernel_call(
        optional(outer_body, [True] * 8 + [True, two_cols] + [True, two_rows] * 2),
        [shifted(4), shifted(4), half, half],
        [pltpu.VMEM((2, 4, 3 * ch, cols), BF)],
        flops=1 << 28,
        name="outer",
    )(wf, x16, own, xi, xc, hids, g1, g2, *strips, *got_rows, *corners)

    def back(kernel, mid, ends, flip, name):
        return kernel_call(
            functools.partial(back_body, flip),
            [sds(images.shape, BF)],
            [
                pltpu.VMEM((2 * ch, 12 * ch), BF),
                pltpu.VMEM((halves, (ch + 1) * pitch, LANES), F32),
            ],
            flops=1 << 29,
            name=name,
        )(kernel, mid, ends)[0]

    partner = [(i, i ^ 1) for i in range(n_dp)]
    total_half = mine + lax.ppermute(other, "dp", partner)
    steps = [(0, 1 << k) for k in range(1, n_dp.bit_length() - 1)]
    steps += [(1, 1 << k) for k in range(n_row.bit_length() - 1)]
    steps += [(2, 1 << k) for k in range(n_col.bit_length() - 1)]
    out = back(taps2, acts, acts_o, False, "out")
    grad_in = back(taps1, hids, hids_o, True, "grad_in")
    stages = [steps[k : k + 2] for k in range(0, len(steps), 2)]
    for k, stage in enumerate(stages):
        total_half = exchange(total_half, stage)
        if k == len(stages) - 2:
            total_half, out = lax.optimization_barrier((total_half, out))
        if k == len(stages) - 1:
            total_half, grad_in = lax.optimization_barrier((total_half, grad_in))
    rest = lax.ppermute(total_half, "dp", partner)
    taps = sds((3, 3, ch, ch), F32)
    first, second = kernel_call(
        functools.partial(finish_body, factor), [taps, taps], name="finish"
    )(total_half, rest)
    return out, grad_in, first.transpose(2, 3, 0, 1), second.transpose(2, 3, 0, 1)


def solution(mesh):
    in_specs = (P("dp", None, "row", "col"), P(), P(), P("dp", None, "row", "col"))
    out_specs = (P("dp", None, "row", "col"), P("dp", None, "row", "col"), P(), P())
    return jax.shard_map(
        on_device, mesh=mesh, in_specs=in_specs, out_specs=out_specs, check_vma=False
    )
```
